512 devices in a mesh: win: 128 (over z, y, core), tile: 4 (over x).
Axes of the slice: x: 4, y: 8, z: 8, core: 2. Of those that a mesh axis runs over, the one named last changes fastest.
Arguments:
- right_side: float32 [128, 2, 128, 1024], P('win', None, 'tile'), may hold values from -64 to 64
- error_weight: float32 [128, 2, 128, 1024], P('win', None, 'tile'), may hold values from 0.5 to 4
- coeffs: float32 [4, 128, 2, 128, 1024], P(None, 'win', None, 'tile'), may hold values from 0.1 to 0.4
- obs_block: int32 [128, 128], P('win', 'tile'), may hold values from 0 to 511
- obs_pos: int32 [128, 128, 128], P('win', 'tile'), may hold values from 0 to 127
- obs_weight: float32 [128, 128, 128], P('win', 'tile'), may hold values from 0.5 to 4
Outputs:
- solution_field: float32 [128, 2, 128, 1024], P('win', None, 'tile')
- residual: float32 [128, 2, 128, 1024], P('win', None, 'tile')
The draws below stay inside these ranges and needn't reach their ends.
All inputs are finite; a program needn't handle non-finite values.
Results may differ from the reference program's by a relative error of at most 0.0001.
Values sent between devices are 32-bit elements; how exact they have to be, the bound alone decides.
No kernel may reach another device: no remote copies, remote signals or barrier semaphores. Data moves between devices by JAX's collectives and lax.ppermute only.
A program may use at most 64 MiB of HBM per device.

```python
import math
import jax
import jax.numpy as jnp

LEV = 2
TY = 32
NX = 1024
NBLK = 32
OBSW = 128
ITERS = 3
NWIN = 128
NY = 128
BROWS = 512
N_TILE = 4


def draw_right_side(key, part):
    gaussian = jax.random.normal(jax.random.fold_in(key, 11), (NWIN, LEV, NY, NX), jnp.float32)
    gaussian = jnp.clip(gaussian, -6.0, 6.0)
    growth = 1.0 + 2.0 * jnp.arange(NWIN, dtype=jnp.float32) / max(NWIN - 1, 1)
    growth = growth.reshape(NWIN, 1, 1, 1)
    return growth * gaussian


def place_ends(entries, own_key, low, top_value):
    longest = entries.shape.index(max(entries.shape))
    spots = []
    for shift in (0, 1):
        where = [jax.random.randint(jax.random.fold_in(own_key, axis), (), 0, length) for axis, length in enumerate(entries.shape)]
        where[longest] = (where[longest] + shift) % entries.shape[longest]
        spots.append(tuple(where))
    return entries.at[spots[0]].set(low).at[spots[1]].set(top_value)


def block_levels(key, extent, pieces, smallest, largest):
    def one(axis_at, shards_of):
        heights = jax.random.uniform(jax.random.fold_in(jax.random.fold_in(key, 6), axis_at), (shards_of,), jnp.float32, smallest / len(pieces), largest / len(pieces))
        return jnp.repeat(jnp.exp(heights), extent[axis_at] // shards_of).reshape((-1,) + (1,) * (len(extent) - axis_at - 1))

    level = one(*pieces[0])
    for cut in pieces[1:]:
        level = level * one(*cut)
    return level


def setup_inputs(seed: int = 0) -> dict:
    seeds = jax.random.split(jax.random.key(seed), 7)
    right_side = draw_right_side(jax.random.fold_in(seeds[6], 71), 0)
    error_weight = jnp.clip(jnp.exp(math.log(4.0) - 2.0794415 * jax.random.uniform(seeds[1], (NWIN, LEV, NY, NX), jnp.float32) ** block_levels(seeds[1], (NWIN, LEV, NY, NX), ((0, 128), (2, 4)), -0.2, 0.2)), 0.5, 4.0)
    coeffs = jnp.clip(0.1 + 0.3 * jax.random.uniform(seeds[2], (4, NWIN, LEV, NY, NX), jnp.float32) ** block_levels(seeds[2], (4, NWIN, LEV, NY, NX), ((1, 128), (3, 4)), -0.2, 0.2), 0.1, 0.4)
    obs_block = place_ends(jax.random.randint(seeds[3], (NWIN, N_TILE * NBLK), 0, BROWS), jax.random.fold_in(seeds[3], 1), 0, BROWS - 1).astype(jnp.int32)
    obs_pos = place_ends(jax.random.randint(seeds[4], (NWIN, N_TILE * NBLK, OBSW), 0, OBSW), jax.random.fold_in(seeds[4], 1), 0, OBSW - 1).astype(jnp.int32)
    obs_weight = jnp.clip(jnp.exp(math.log(4.0) - 2.0794415 * jax.random.uniform(seeds[5], (NWIN, N_TILE * NBLK, OBSW), jnp.float32) ** block_levels(seeds[5], (NWIN, N_TILE * NBLK, OBSW), ((0, 128), (1, 4)), -0.2, 0.2)), 0.5, 4.0)
    return {"right_side": right_side, "error_weight": error_weight, "coeffs": coeffs, "obs_block": obs_block, "obs_pos": obs_pos, "obs_weight": obs_weight}


def model_step(state, coeffs):
    padded = jnp.pad(state, ((0, 0), (0, 0), (1, 1), (0, 0)))
    north_south = padded[:, :, 2:, :] + padded[:, :, :-2, :]
    return (coeffs[0] * state + coeffs[1] * north_south
            + coeffs[2] * jnp.roll(state, -1, axis=3) + coeffs[3] * jnp.roll(state, 1, axis=3))


def model_adjoint(state, coeffs):
    spread = jnp.pad(coeffs[1] * state, ((0, 0), (0, 0), (1, 1), (0, 0)))
    north_south = spread[:, :, 2:, :] + spread[:, :, :-2, :]
    return (coeffs[0] * state + north_south
            + jnp.roll(coeffs[2] * state, 1, axis=3) + jnp.roll(coeffs[3] * state, -1, axis=3))


def observe(state, obs_block, obs_pos, obs_weight):
    windows = state.shape[0]
    cell_count = LEV * TY * NX
    blocks = state.reshape(windows, LEV, N_TILE, TY, NX).transpose(0, 2, 1, 3, 4).reshape(windows, N_TILE, cell_count)
    flat_index = (obs_block.reshape(windows, N_TILE, NBLK, 1).astype(jnp.int32) * OBSW
                  + obs_pos.reshape(windows, N_TILE, NBLK, OBSW).astype(jnp.int32))
    flat_index = flat_index.reshape(windows, N_TILE, NBLK * OBSW).astype(jnp.int32)
    observed = jnp.take_along_axis(blocks, flat_index, axis=2)
    weighted = observed * obs_weight.reshape(windows, N_TILE, NBLK * OBSW)

    def place(index_row, value_row):
        return jnp.zeros((cell_count,), jnp.float32).at[index_row].add(value_row)

    spread = jax.vmap(jax.vmap(place))(flat_index, weighted)
    return spread.reshape(windows, N_TILE, LEV, TY, NX).transpose(0, 2, 1, 3, 4).reshape(windows, LEV, NY, NX)


def reference(right_side, error_weight, coeffs, obs_block, obs_pos, obs_weight):
    def hessian(state):
        propagated = model_step(state, coeffs)
        before = jnp.concatenate([jnp.zeros_like(propagated[:1]), propagated[:-1]], axis=0)
        weighted = error_weight * (state - before)
        following = jnp.concatenate([weighted[1:], jnp.zeros_like(weighted[:1])], axis=0)
        return weighted - model_adjoint(following, coeffs) + observe(state, obs_block, obs_pos, obs_weight)

    solution_field = jnp.zeros_like(right_side)
    residual = right_side
    direction = right_side
    norm_now = jnp.sum(residual * residual)
    for iteration in range(ITERS):
        product_vec = hessian(direction)
        step_length = norm_now / jnp.sum(direction * product_vec)
        solution_field = solution_field + step_length * direction
        residual = residual - step_length * product_vec
        norm_next = jnp.sum(residual * residual)
        direction = residual + (norm_next / norm_now) * direction
        norm_now = norm_next
    return solution_field, residual
```

```python
import jax
import jax.numpy as jnp
from jax import lax
from jax.experimental import pallas as pl
from jax.experimental.pallas import tpu as pltpu
from jax.sharding import Mesh
from jax.sharding import PartitionSpec as P

WIN = ("win_0", "win_1", "win_2")
THETA = 6.0
G = 8
HALO = 6
F32 = jnp.float32


def call(body, out_shape, aliases=None, smem=(), count=0, scratch=()):
    specs = [
        pl.BlockSpec(memory_space=pltpu.SMEM if i in smem else pltpu.VMEM) for i in range(count)
    ]
    outs = [pl.BlockSpec(memory_space=pltpu.VMEM) for _ in out_shape]
    return pl.pallas_call(
        body,
        out_shape=out_shape,
        in_specs=specs,
        out_specs=outs,
        scratch_shapes=scratch,
        input_output_aliases=aliases or {},
        compiler_params=pltpu.CompilerParams(vmem_limit_bytes=24 * 2**20),
    )


def shape(*dims):
    return jax.ShapeDtypeStruct(dims, F32)


def west(x):
    return pltpu.roll(x, 1, axis=1)


def east(x):
    return pltpu.roll(x, x.shape[1] - 1, axis=1)


def north_of(ref, lev, tile):
    if tile == 0:
        return pltpu.roll(ref[lev, 0:8, :], 1, axis=0)
    return ref[lev, 8 * tile - 1 : 8 * tile + 7, :]


def south_of(ref, lev, tile, tiles):
    if tile == tiles - 1:
        return pltpu.roll(ref[lev, 8 * tile : 8 * tile + 8, :], 7, axis=0)
    return ref[lev, 8 * tile + 1 : 8 * tile + 9, :]


def folded(x):
    total = x[:, 0:128]
    for at in range(128, x.shape[1], 128):
        total = total + x[:, at : at + 128]
    return total


PARTS = (("b", HALO), ("c", HALO - 1), ("w", HALO - 1), ("d", HALO - 2))
PER_LEVEL = HALO + 5 * (HALO - 1) + (HALO - 2)


def message_rows(levels):
    return -(-levels * PER_LEVEL // 8) * 8


def ghost_items(levels):
    at = 0
    for lev in range(levels):
        for name, rows in PARTS:
            for f in range(4 if name == "c" else 1):
                yield name, f, lev, at, rows
                at += rows


def pack_kernel(b, c, w, pos, block, weight, north, south, d, blocks):
    levels, rows, width = b.shape
    per_row = width // 128
    pos_all, weight_all = pos[...], weight[...]
    n = pos_all.shape[0]
    cell = lax.broadcasted_iota(jnp.int32, (n, 128), 1)
    sums = [jnp.zeros((n, 128), F32) for _ in range(4)]
    for j in range(pos_all.shape[1]):
        here = jnp.broadcast_to(pos_all[:, j : j + 1], (n, 128))
        value = jnp.broadcast_to(weight_all[:, j : j + 1], (n, 128))
        sums[j % 4] = sums[j % 4] + jnp.where(here == cell, value, 0.0)
    hot = (sums[0] + sums[1]) + (sums[2] + sums[3])
    blocks[...] = jnp.zeros(blocks.shape, F32)
    for i in range(n):
        at = pl.ds(block[0, i], 1)
        blocks[at, :] = blocks[at, :] + hot[i : i + 1, :]
    for j in range(per_row):
        d[:, j * 128 : j * 128 + 128] = blocks[pl.ds(j, levels * rows, stride=per_row), :]
    for name, f, lev, at, count in ghost_items(levels):
        for out, first in ((north, 0), (south, rows - count)):
            if name == "d":
                piece = d[lev * rows + first : lev * rows + first + count, :]
            elif name == "c":
                piece = c[f, lev, first : first + count, :]
            else:
                piece = (b if name == "b" else w)[lev, first : first + count, :]
            out[at : at + count, :] = piece
    used = levels * PER_LEVEL
    for out in (north, south):
        if out.shape[0] > used:
            out[used:, :] = jnp.zeros((out.shape[0] - used, width), F32)


def extend_kernel(b, c, w, d, b_e, c_e, w_e, d_e):
    levels, rows, width = b.shape
    blank = jnp.zeros((G, width), F32)
    for lev in range(levels):
        targets = [(b_e.at[lev], b.at[lev]), (w_e.at[lev], w.at[lev])]
        targets += [(c_e.at[f, lev], c.at[f, lev]) for f in range(4)]
        targets += [(d_e.at[lev], d.at[lev * rows : (lev + 1) * rows])]
        for out, src in targets:
            out[0:G, :] = blank
            out[G : G + rows, :] = src[...]
            out[G + rows :, :] = blank


def model_tile(q, c, lev, tile, tiles):
    here = q[lev, 8 * tile : 8 * tile + 8, :]
    at = slice(8 * tile, 8 * tile + 8)
    return (
        c[0, lev, at, :] * here
        + c[1, lev, at, :] * (north_of(q, lev, tile) + south_of(q, lev, tile, tiles))
        + c[2, lev, at, :] * east(here)
        + c[3, lev, at, :] * west(here)
    )


def propagate(q, c, p):
    levels, rows, _ = q.shape
    for lev in range(levels):
        for tile in range(rows // 8):
            p[lev, 8 * tile : 8 * tile + 8, :] = model_tile(q, c, lev, tile, rows // 8)


def post(out, values, lev):
    rows = out.shape[1]
    out[lev, :, :] = values[lev, 4 : 4 + rows, :]


def core_is_one():
    return lax.axis_index("win_2") == 1


def ghosts_kernel(from_north, from_south, b_in, c_in, w_in, d_in, b_e, c_e, w_e, d_e, p, cross, within):
    levels, total, width = b_e.shape
    rows = total - 2 * G
    for name, f, lev, at, count in ghost_items(levels):
        out = {"b": b_e, "w": w_e, "d": d_e}.get(name)
        out = c_e.at[f] if out is None else out
        out[lev, G - count : G, :] = from_north[at : at + count, :]
        out[lev, G + rows : G + rows + count, :] = from_south[at : at + count, :]
    propagate(b_e, c_e, p)

    def send(forward, backward):
        for lev in range(levels):
            post(forward, p, lev)
            for f, field in enumerate((b_e, w_e)):
                backward[lev, 16 * f : 16 * f + 8, :] = field[lev, 0:8, :]
                backward[lev, 16 * f + 8 : 16 * f + 16, :] = field[lev, G + rows :, :]
            backward[lev, 32:40, :] = jnp.zeros((8, width), F32)

    @pl.when(core_is_one())
    def _():
        send(cross, within)

    @pl.when(jnp.logical_not(core_is_one()))
    def _():
        send(within, cross)


def unposted(ref, lev, tile, tiles):
    if tile == 0:
        return pltpu.roll(ref[lev, 0:8, :], 4, axis=0)
    if tile == tiles - 1:
        return pltpu.roll(ref[lev, 8 * tile - 8 : 8 * tile, :], 4, axis=0)
    return ref[lev, 8 * tile - 4 : 8 * tile + 4, :]


def second_half(q, c, w, d, p, v_next, w_next, p_prev, out, edge):
    levels, total, _ = q.shape
    tiles = total // 8
    for lev in range(levels):
        for tile in range(tiles):
            at = slice(8 * tile, 8 * tile + 8)
            here, weight = q[lev, at, :], w[lev, at, :]
            following = w_next(lev, tile) * (v_next(lev, tile) - p[lev, at, :])
            edge[lev, at, :] = c[1, lev, at, :] * following
            out[lev, at, :] = (
                (weight + d[lev, at, :] - THETA) * here
                - weight * p_prev(lev, tile)
                - c[0, lev, at, :] * following
                - west(c[2, lev, at, :] * following)
                - east(c[3, lev, at, :] * following)
            )
    for lev in range(levels):
        for tile in range(tiles):
            at = slice(8 * tile, 8 * tile + 8)
            value = out[lev, at, :] - (north_of(edge, lev, tile) + south_of(edge, lev, tile, tiles))
            if tile in (0, tiles - 1):
                value = jnp.where(w[lev, at, :] > 0.0, value, 0.0)
            out[lev, at, :] = value


def products(pairs, levels, tiles, out):
    for i, (x, y) in enumerate(pairs):
        total = jnp.zeros((8, 128), F32)
        for lev in range(levels):
            for tile in range(1, tiles - 1):
                at = slice(8 * tile, 8 * tile + 8)
                total = total + folded(x[lev, at, :] * y[lev, at, :])
        out[i] = total


def send_both(q, p, cross, within):
    def send(forward, backward):
        for lev in range(q.shape[0]):
            post(forward, p, lev)
            post(backward, q, lev)

    @pl.when(core_is_one())
    def _():
        send(cross, within)

    @pl.when(jnp.logical_not(core_is_one()))
    def _():
        send(within, cross)


def first_apply_kernel(
    b_e, c, w, d, p0, b_next, w_next_own, cross_in, within_in,
    q1, p1, w_next, cross, within, sums, edge,
):
    levels, total, width = b_e.shape
    tiles = total // 8
    one = core_is_one()

    def edge_tile(f, lev, tile):
        at = 16 * f + (0 if tile == 0 else 8)
        return jnp.where(one, cross_in[lev, at : at + 8, :], within_in[lev, at : at + 8, :])

    for lev in range(levels):
        for tile in range(tiles):
            at = slice(8 * tile, 8 * tile + 8)
            if tile in (0, tiles - 1):
                w_next[lev, at, :] = edge_tile(1, lev, tile)
            else:
                w_next[lev, at, :] = w_next_own[lev, 8 * tile - G : 8 * tile - G + 8, :]

    def v_next(lev, tile):
        if tile in (0, tiles - 1):
            return edge_tile(0, lev, tile)
        return b_next[lev, 8 * tile - G : 8 * tile - G + 8, :]

    def p_prev(lev, tile):
        return jnp.where(
            one, unposted(within_in, lev, tile, tiles), unposted(cross_in, lev, tile, tiles)
        )

    second_half(
        b_e, c, w, d, p0, v_next,
        lambda lev, tile: w_next[lev, 8 * tile : 8 * tile + 8, :], p_prev, q1, edge,
    )
    propagate(q1, c, p1)
    send_both(q1, p1, cross, within)
    products(((b_e, b_e), (b_e, q1), (q1, q1)), levels, tiles, sums)


def apply_kernel(
    q1, c, w, d, p1, w_next, cross_in, within_in, q2, p2, cross, within, sums, edge
):
    levels, total, width = q1.shape
    tiles = total // 8
    one = core_is_one()

    def v_next(lev, tile):
        return jnp.where(
            one, unposted(cross_in, lev, tile, tiles), unposted(within_in, lev, tile, tiles)
        )

    def p_prev(lev, tile):
        return jnp.where(
            one, unposted(within_in, lev, tile, tiles), unposted(cross_in, lev, tile, tiles)
        )

    second_half(
        q1, c, w, d, p1, v_next,
        lambda lev, tile: w_next[lev, 8 * tile : 8 * tile + 8, :], p_prev, q2, edge,
    )
    propagate(q2, c, p2)
    send_both(q2, p2, cross, within)
    products(((q1, q2), (q2, q2)), levels, tiles, sums)


def moments_kernel(q2, c, w, d, p2, w_next, cross_in, within_in, sums_1, sums_2, out, q3, edge):
    levels, total, width = q2.shape
    tiles = total // 8
    one = core_is_one()
    first = jnp.logical_and(
        lax.axis_index("win_0") + lax.axis_index("win_1") == 0, jnp.logical_not(one)
    )

    def v_next(lev, tile):
        return jnp.where(
            one, unposted(cross_in, lev, tile, tiles), unposted(within_in, lev, tile, tiles)
        )

    def p_prev(lev, tile):
        return jnp.where(
            one, unposted(within_in, lev, tile, tiles), unposted(cross_in, lev, tile, tiles)
        )

    last = jnp.zeros((8, 128), F32)
    for lev in range(levels):
        for tile in range(1, tiles - 1):
            at = slice(8 * tile, 8 * tile + 8)
            here = q2[lev, at, :]
            gap = v_next(lev, tile) - p2[lev, at, :]
            own = d[lev, at, :] - THETA + jnp.where(first, w[lev, at, :], 0.0)
            last = last + folded(w_next[lev, at, :] * gap * gap + own * here * here)
    row = lax.broadcasted_iota(jnp.int32, (8, 128), 0)
    result = jnp.zeros((8, 128), F32)
    for i, part in enumerate([sums_1[0], sums_1[1], sums_1[2], sums_2[0], sums_2[1], last]):
        total_i = jnp.sum(part, axis=0, keepdims=True)
        result = jnp.where(row == i, jnp.broadcast_to(total_i, (8, 128)), result)
    for i in range(out.shape[0]):
        out[i] = result
    second_half(
        q2, c, w, d, p2, v_next,
        lambda lev, tile: w_next[lev, 8 * tile : 8 * tile + 8, :], p_prev, q3, edge,
    )


def spread_kernel(x, out):
    total = x[0]
    for i in range(1, x.shape[0]):
        total = total + x[i]
    for i in range(out.shape[0]):
        out[i] = total


def times_a(v):
    longer = [THETA * x for x in v] + [0.0]
    return [longer[i] + (v[i - 1] if i else 0.0) for i in range(len(longer))]


def inner(u, v, mu):
    return sum(x * y * mu[i + j] for i, x in enumerate(u) for j, y in enumerate(v))


def plus(u, scale, v):
    size = max(len(u), len(v))
    u, v = u + [0.0] * (size - len(u)), v + [0.0] * (size - len(v))
    return [x + scale * y for x, y in zip(u, v)]


def coordinates(mu, iters=3):
    x, r, p = [0.0], [1.0], [1.0]
    rr = mu[0]
    for i in range(iters):
        image = times_a(p)
        alpha = rr / inner(p, image, mu)
        x = plus(x, alpha, p)
        r = plus(r, -alpha, image)
        if i + 1 < iters:
            new = inner(r, r, mu)
            p = plus(r, new / rr, p)
            rr = new
    return x, r


def finish_kernel(parts, q0, q1, q2, q3, solution_field, residual):
    levels, rows, width = solution_field.shape
    total = parts[0]
    for i in range(1, parts.shape[0]):
        total = total + parts[i]
    summed = jnp.sum(total, axis=1, keepdims=True)
    mu = [jnp.broadcast_to(summed[i : i + 1, :], (8, 128)) for i in range(6)]
    x, r = coordinates(mu)
    wide = lambda v: jnp.concatenate([v] * (width // 128), axis=1)
    x = [wide(v) for v in x]
    r = [wide(v) for v in r]
    for lev in range(levels):
        for at in range(0, rows, 8):
            s = [q[lev, G + at : G + at + 8, :] for q in (q0, q1, q2, q3)]
            solution_field[lev, at : at + 8, :] = x[0] * s[0] + x[1] * s[1] + x[2] * s[2]
            residual[lev, at : at + 8, :] = r[0] * s[0] + r[1] * s[1] + r[2] * s[2] + r[3] * s[3]


def shifted(x, axis, by):
    count = lax.axis_size(axis)
    return lax.ppermute(x, axis, [(i, i + by) for i in range(count) if 0 <= i + by < count])


def over_chips(x):
    count = lax.axis_size(WIN)
    pairs = [(i, i + 1) for i in range(1, count - 1, 2)]
    return lax.ppermute(x, WIN, pairs + [(b, a) for a, b in pairs])


def on_chip(x):
    return lax.ppermute(x, "win_2", [(0, 1), (1, 0)])


def on_device(right_side, error_weight, coeffs, obs_block, obs_pos, obs_weight):
    b, w, c = right_side[0], error_weight[0], coeffs[:, 0]
    levels, rows, width = b.shape
    total = rows + 2 * G
    field = shape(levels, total, width)
    ghost = shape(message_rows(levels), width)
    message = shape(levels, 40, width)

    north, south, d = call(
        pack_kernel,
        [ghost, ghost, shape(levels * rows, width)],
        smem=(4,),
        count=6,
        scratch=(pltpu.VMEM((b.size // 128, 128), F32),),
    )(b, c, w, obs_pos[0], obs_block, obs_weight[0])
    from_south = shifted(north, "tile", -1)
    from_north = shifted(south, "tile", 1)
    b_next = shifted(b, WIN, -1)
    w_next_own = shifted(w, WIN, -1)
    b_e, c_e, w_e, d_e = call(
        extend_kernel, [field, shape(4, levels, total, width), field, field], count=4
    )(b, c, w, d)
    b_e, c_e, w_e, d_e, p0, cross, within = call(
        ghosts_kernel,
        [field, shape(4, levels, total, width), field, field, field, message, message],
        aliases={2: 0, 3: 1, 4: 2, 5: 3},
        count=6,
    )(from_north, from_south, b_e, c_e, w_e, d_e)
    cross, within = over_chips(cross), on_chip(within)
    scratch = (pltpu.VMEM((levels, total, width), F32),)
    q1, p1, w_next, cross, within, sums_1 = call(
        first_apply_kernel,
        [field, field, field, message, message, shape(3, 8, 128)],
        count=9,
        scratch=scratch,
    )(b_e, c_e, w_e, d_e, p0, b_next, w_next_own, cross, within)
    cross, within = over_chips(cross), on_chip(within)
    q2, p2, cross, within, sums_2 = call(
        apply_kernel,
        [field, field, message, message, shape(2, 8, 128)],
        count=8,
        scratch=scratch,
    )(q1, c_e, w_e, d_e, p1, w_next, cross, within)
    cross, within = over_chips(cross), on_chip(within)
    near, far = ("win_2", "tile"), ("win_0", "win_1")
    moments, q3 = call(
        moments_kernel, [shape(lax.axis_size(near), 8, 128), field], count=10, scratch=scratch
    )(q2, c_e, w_e, d_e, p2, w_next, cross, within, sums_1, sums_2)
    moments = lax.all_to_all(moments, near, 0, 0, tiled=True)
    (moments,) = call(spread_kernel, [shape(lax.axis_size(far), 8, 128)], count=1)(moments)
    moments = lax.all_to_all(moments, far, 0, 0, tiled=True)
    solution_field, residual = call(
        finish_kernel, [shape(levels, rows, width), shape(levels, rows, width)], count=5
    )(moments, b_e, q1, q2, q3)
    return solution_field[None], residual[None]


def solution(mesh):
    split = Mesh(
        mesh.devices.reshape(8, 8, 2, mesh.shape["tile"]), ("win_0", "win_1", "win_2", "tile")
    )
    in_specs = (
        P(WIN, None, "tile", None),
        P(WIN, None, "tile", None),
        P(None, WIN, None, "tile", None),
        P(WIN, "tile"),
        P(WIN, "tile", None),
        P(WIN, "tile", None),
    )
    out_specs = (P(WIN, None, "tile", None), P(WIN, None, "tile", None))
    return jax.shard_map(
        on_device, mesh=split, in_specs=in_specs, out_specs=out_specs, check_vma=False
    )
```

```python
import jax
import jax.numpy as jnp
from jax import lax
from jax.experimental import pallas as pl
from jax.experimental.pallas import tpu as pltpu
from jax.sharding import Mesh
from jax.sharding import PartitionSpec as P


WIN = ("win_0", "win_1", "win_2")
THETA = 6.0
G = 8
HALO = 6
F32 = jnp.float32


def call(body, out_shape, aliases=None, hbm=False, count=0, scratch=()):
    place = pltpu.HBM if hbm else pltpu.VMEM
    return pl.pallas_call(
        body,
        out_shape=out_shape,
        in_specs=[pl.BlockSpec(memory_space=place) for _ in range(count)],
        out_specs=[pl.BlockSpec(memory_space=pltpu.VMEM) for _ in out_shape],
        scratch_shapes=scratch,
        input_output_aliases=aliases or {},
        compiler_params=pltpu.CompilerParams(vmem_limit_bytes=24 * 2**20),
    )


def in_hbm(x):
    return pltpu.with_memory_space_constraint(x, pltpu.HBM)


def shape(*dims):
    return jax.ShapeDtypeStruct(dims, F32)


def west(x):
    return pltpu.roll(x, 1, axis=1)


def east(x):
    return pltpu.roll(x, x.shape[1] - 1, axis=1)


def north_of(ref, lev, tile):
    if tile == 0:
        return pltpu.roll(ref[lev, 0:8, :], 1, axis=0)
    return ref[lev, 8 * tile - 1 : 8 * tile + 7, :]


def south_of(ref, lev, tile, tiles):
    if tile == tiles - 1:
        return pltpu.roll(ref[lev, 8 * tile : 8 * tile + 8, :], 7, axis=0)
    return ref[lev, 8 * tile + 1 : 8 * tile + 9, :]


def folded(x):
    total = x[:, 0:128]
    for at in range(128, x.shape[1], 128):
        total = total + x[:, at : at + 128]
    return total


PARTS = (("b", HALO), ("c", HALO - 1), ("w", HALO - 1), ("d", HALO - 2))
PER_LEVEL = HALO + 5 * (HALO - 1) + (HALO - 2)


EDGES = 20


def message_rows(levels):
    return -(-levels * PER_LEVEL // 8) * 8


def ghost_items(levels):
    at = 0
    for lev in range(levels):
        for name, rows in PARTS:
            for f in range(4 if name == "c" else 1):
                yield name, f, lev, at, rows
                at += rows


def pack_kernel(
    b_hbm, c_hbm, w_hbm, pos_hbm, block_hbm, weight_hbm,
    north, south, b_e, c_e, w_e, d_e, cross, within,
    pos, block, weight, blocks, sems,
):
    levels, rows, width = b_hbm.shape
    per_row = width // 128
    own = pl.ds(G, rows)
    moves = [
        pltpu.make_async_copy(src, dst, sems.at[i])
        for i, (src, dst) in enumerate(
            (
                (pos_hbm, pos),
                (weight_hbm, weight),
                (block_hbm, block),
                (b_hbm, b_e.at[:, own, :]),
                (c_hbm, c_e.at[:, :, own, :]),
                (w_hbm, w_e.at[:, own, :]),
            )
        )
    ]
    for move in moves:
        move.start()
    blank = jnp.zeros((G, width), F32)
    for lev in range(levels):
        for out in (b_e.at[lev], w_e.at[lev], d_e.at[lev], *(c_e.at[f, lev] for f in range(4))):
            out[0:G, :] = blank
            out[G + rows :, :] = blank
    blocks[...] = jnp.zeros(blocks.shape, F32)
    for move in moves[:3]:
        move.wait()
    pos_all, weight_all = pos[...], weight[...]
    n = pos_all.shape[0]
    cell = lax.broadcasted_iota(jnp.int32, (n, 128), 1)
    sums = [jnp.zeros((n, 128), F32) for _ in range(4)]
    for j in range(pos_all.shape[1]):
        here = jnp.broadcast_to(pos_all[:, j : j + 1], (n, 128))
        value = jnp.broadcast_to(weight_all[:, j : j + 1], (n, 128))
        sums[j % 4] = sums[j % 4] + jnp.where(here == cell, value, 0.0)
    hot = (sums[0] + sums[1]) + (sums[2] + sums[3])
    for i in range(n):
        at = pl.ds(block[0, i], 1)
        blocks[at, :] = blocks[at, :] + hot[i : i + 1, :]
    for lev in range(levels):
        for j in range(per_row):
            first = lev * rows * per_row + j
            d_e[lev, G : G + rows, j * 128 : j * 128 + 128] = blocks[
                pl.ds(first, rows, stride=per_row), :
            ]
    for move in moves[3:]:
        move.wait()
    for name, f, lev, at, count in ghost_items(levels):
        src = {"b": b_e, "w": w_e, "d": d_e}.get(name)
        src = c_e.at[f] if src is None else src
        north[at : at + count, :] = src[lev, G : G + count, :]
        south[at : at + count, :] = src[lev, G + rows - count : G + rows, :]
    used = levels * PER_LEVEL
    for out in (north, south):
        if out.shape[0] > used:
            out[used:, :] = jnp.zeros((out.shape[0] - used, width), F32)

    def send(forward, backward):
        for lev in range(levels):
            backward[lev, :, :] = b_e[lev, G : G + rows, :]
            for tile in range(1, 1 + rows // 8):
                at = 8 * tile - G
                forward[lev, at : at + 8, :] = model_tile(b_e, c_e, lev, tile, 2 + rows // 8)

    @pl.when(core_is_one())
    def _():
        send(cross, within)

    @pl.when(jnp.logical_not(core_is_one()))
    def _():
        send(within, cross)


def model_tile(q, c, lev, tile, tiles):
    here = q[lev, 8 * tile : 8 * tile + 8, :]
    at = slice(8 * tile, 8 * tile + 8)
    return (
        c[0, lev, at, :] * here
        + c[1, lev, at, :] * (north_of(q, lev, tile) + south_of(q, lev, tile, tiles))
        + c[2, lev, at, :] * east(here)
        + c[3, lev, at, :] * west(here)
    )


def propagate(q, c, p):
    levels, rows, _ = q.shape
    for lev in range(levels):
        for tile in range(rows // 8):
            p[lev, 8 * tile : 8 * tile + 8, :] = model_tile(q, c, lev, tile, rows // 8)


def post(out, values, lev):
    rows = out.shape[1]
    out[lev, :, :] = values[lev, 4 : 4 + rows, :]


def core_is_one():
    return lax.axis_index("win_2") == 1


def ghosts_kernel(from_north, from_south, b_in, c_in, w_in, d_in, b_e, c_e, w_e, d_e, p, cross, within):
    levels, total, width = b_e.shape
    rows = total - 2 * G
    for name, f, lev, at, count in ghost_items(levels):
        out = {"b": b_e, "w": w_e, "d": d_e}.get(name)
        out = c_e.at[f] if out is None else out
        out[lev, G - count : G, :] = from_north[at : at + count, :]
        out[lev, G + rows : G + rows + count, :] = from_south[at : at + count, :]
    propagate(b_e, c_e, p)

    def send(forward, backward):
        for lev in range(levels):
            at = lev * EDGES
            for f, (field, first) in enumerate(((b_e, 3), (w_e, 3))):
                low, high = at + 10 * f, at + 10 * f + 5
                backward[low : low + 5, :] = field[lev, first : first + 5, :]
                backward[high : high + 5, :] = field[lev, G + rows : G + rows + 5, :]
            forward[at : at + 5, :] = p[lev, 4:9, :]
            forward[at + 5 : at + 10, :] = p[lev, G + rows - 1 : G + rows + 4, :]
            forward[at + 10 : at + EDGES, :] = jnp.zeros((EDGES - 10, width), F32)

    @pl.when(core_is_one())
    def _():
        send(cross, within)

    @pl.when(jnp.logical_not(core_is_one()))
    def _():
        send(within, cross)


def unposted(ref, lev, tile, tiles):
    if tile == 0:
        return pltpu.roll(ref[lev, 0:8, :], 4, axis=0)
    if tile == tiles - 1:
        return pltpu.roll(ref[lev, 8 * tile - 8 : 8 * tile, :], 4, axis=0)
    return ref[lev, 8 * tile - 4 : 8 * tile + 4, :]


def second_half(q, c, w, d, p, v_next, w_next, p_prev, out, edge):
    levels, total, _ = q.shape
    tiles = total // 8
    for lev in range(levels):
        for tile in range(tiles):
            at = slice(8 * tile, 8 * tile + 8)
            here, weight = q[lev, at, :], w[lev, at, :]
            following = w_next(lev, tile) * (v_next(lev, tile) - p[lev, at, :])
            edge[lev, at, :] = c[1, lev, at, :] * following
            out[lev, at, :] = (
                (weight + d[lev, at, :] - THETA) * here
                - weight * p_prev(lev, tile)
                - c[0, lev, at, :] * following
                - west(c[2, lev, at, :] * following)
                - east(c[3, lev, at, :] * following)
            )
    for lev in range(levels):
        for tile in range(tiles):
            at = slice(8 * tile, 8 * tile + 8)
            value = out[lev, at, :] - (north_of(edge, lev, tile) + south_of(edge, lev, tile, tiles))
            if tile in (0, tiles - 1):
                value = jnp.where(w[lev, at, :] > 0.0, value, 0.0)
            out[lev, at, :] = value


def products(pairs, levels, tiles, out):
    for i, (x, y) in enumerate(pairs):
        total = jnp.zeros((8, 128), F32)
        for lev in range(levels):
            for tile in range(1, tiles - 1):
                at = slice(8 * tile, 8 * tile + 8)
                total = total + folded(x[lev, at, :] * y[lev, at, :])
        out[i] = total


def send_both(q, p, cross, within):
    def send(forward, backward):
        for lev in range(q.shape[0]):
            post(forward, p, lev)
            post(backward, q, lev)

    @pl.when(core_is_one())
    def _():
        send(cross, within)

    @pl.when(jnp.logical_not(core_is_one()))
    def _():
        send(within, cross)


def first_apply_kernel(
    b_e, c, w, d, p0, cross_own, within_own, w_next_own, cross_in, within_in,
    q1, p1, w_next, cross, within, sums, edge, v_next, p_prev,
):
    levels, total, width = b_e.shape
    tiles = total // 8
    rows = total - 2 * G

    def assemble(p_own, v_own, p_edges, v_edges):
        for lev in range(levels):
            at = lev * EDGES
            for out, src in ((p_prev, p_own), (v_next, v_own), (w_next, w_next_own)):
                out[lev, G : G + rows, :] = src[lev, :, :]
            for f, out in enumerate((v_next, w_next)):
                low, high = at + 10 * f, at + 10 * f + 5
                out[lev, 3:8, :] = v_edges[low : low + 5, :]
                out[lev, G + rows : G + rows + 5, :] = v_edges[high : high + 5, :]
            p_prev[lev, 4:9, :] = p_edges[at : at + 5, :]
            p_prev[lev, G + rows - 1 : G + rows + 4, :] = p_edges[at + 5 : at + 10, :]

    blank = jnp.zeros((G, width), F32)
    for lev in range(levels):
        for out in (p_prev, v_next, w_next):
            out[lev, 0:G, :] = blank
            out[lev, G + rows :, :] = blank

    @pl.when(core_is_one())
    def _():
        assemble(within_own, cross_own, within_in, cross_in)

    @pl.when(jnp.logical_not(core_is_one()))
    def _():
        assemble(cross_own, within_own, cross_in, within_in)

    def tile_of(ref):
        return lambda lev, tile: ref[lev, 8 * tile : 8 * tile + 8, :]

    second_half(
        b_e, c, w, d, p0, tile_of(v_next), tile_of(w_next), tile_of(p_prev), q1, edge
    )
    propagate(q1, c, p1)
    send_both(q1, p1, cross, within)
    products(((b_e, b_e), (b_e, q1), (q1, q1)), levels, tiles, sums)


def apply_kernel(
    q1, c, w, d, p1, w_next, cross_in, within_in, q2, p2, cross, within, sums, edge
):
    levels, total, _ = q1.shape
    tiles = total // 8
    one = core_is_one()

    def v_next(lev, tile):
        return jnp.where(
            one, unposted(cross_in, lev, tile, tiles), unposted(within_in, lev, tile, tiles)
        )

    def p_prev(lev, tile):
        return jnp.where(
            one, unposted(within_in, lev, tile, tiles), unposted(cross_in, lev, tile, tiles)
        )

    second_half(
        q1, c, w, d, p1, v_next,
        lambda lev, tile: w_next[lev, 8 * tile : 8 * tile + 8, :], p_prev, q2, edge,
    )
    propagate(q2, c, p2)
    send_both(q2, p2, cross, within)
    products(((q1, q2), (q2, q2)), levels, tiles, sums)


def moments_kernel(q2, c, w, d, p2, w_next, cross_in, within_in, sums_1, sums_2, out, q3, edge):
    levels, total, _ = q2.shape
    tiles = total // 8
    one = core_is_one()
    first = jnp.logical_and(
        lax.axis_index("win_0") + lax.axis_index("win_1") == 0, jnp.logical_not(one)
    )

    def v_next(lev, tile):
        return jnp.where(
            one, unposted(cross_in, lev, tile, tiles), unposted(within_in, lev, tile, tiles)
        )

    def p_prev(lev, tile):
        return jnp.where(
            one, unposted(within_in, lev, tile, tiles), unposted(cross_in, lev, tile, tiles)
        )

    last = jnp.zeros((8, 128), F32)
    for lev in range(levels):
        for tile in range(1, tiles - 1):
            at = slice(8 * tile, 8 * tile + 8)
            here = q2[lev, at, :]
            gap = v_next(lev, tile) - p2[lev, at, :]
            own = d[lev, at, :] - THETA + jnp.where(first, w[lev, at, :], 0.0)
            last = last + folded(w_next[lev, at, :] * gap * gap + own * here * here)
    row = lax.broadcasted_iota(jnp.int32, (8, 128), 0)
    result = jnp.zeros((8, 128), F32)
    for i, part in enumerate([sums_1[0], sums_1[1], sums_1[2], sums_2[0], sums_2[1], last]):
        total_i = jnp.sum(part, axis=0, keepdims=True)
        result = jnp.where(row == i, jnp.broadcast_to(total_i, (8, 128)), result)
    for i in range(out.shape[0]):
        out[i] = result
    second_half(
        q2, c, w, d, p2, v_next,
        lambda lev, tile: w_next[lev, 8 * tile : 8 * tile + 8, :], p_prev, q3, edge,
    )


def spread_kernel(x, out):
    total = x[0]
    for i in range(1, x.shape[0]):
        total = total + x[i]
    for i in range(out.shape[0]):
        out[i] = total


def times_a(v):
    longer = [THETA * x for x in v] + [0.0]
    return [longer[i] + (v[i - 1] if i else 0.0) for i in range(len(longer))]


def inner(u, v, mu):
    return sum(x * y * mu[i + j] for i, x in enumerate(u) for j, y in enumerate(v))


def plus(u, scale, v):
    size = max(len(u), len(v))
    u, v = u + [0.0] * (size - len(u)), v + [0.0] * (size - len(v))
    return [x + scale * y for x, y in zip(u, v)]


def coordinates(mu, iters=3):
    x, r, p = [0.0], [1.0], [1.0]
    rr = mu[0]
    for i in range(iters):
        image = times_a(p)
        alpha = rr / inner(p, image, mu)
        x = plus(x, alpha, p)
        r = plus(r, -alpha, image)
        if i + 1 < iters:
            new = inner(r, r, mu)
            p = plus(r, new / rr, p)
            rr = new
    return x, r


def finish_kernel(parts, q0, q1, q2, q3, solution_field, residual):
    levels, rows, width = solution_field.shape
    total = parts[0]
    for i in range(1, parts.shape[0]):
        total = total + parts[i]
    summed = jnp.sum(total, axis=1, keepdims=True)
    mu = [jnp.broadcast_to(summed[i : i + 1, :], (8, 128)) for i in range(6)]
    x, r = coordinates(mu)
    wide = lambda v: jnp.concatenate([v] * (width // 128), axis=1)
    x = [wide(v) for v in x]
    r = [wide(v) for v in r]
    for lev in range(levels):
        for at in range(0, rows, 8):
            s = [q[lev, G + at : G + at + 8, :] for q in (q0, q1, q2, q3)]
            solution_field[lev, at : at + 8, :] = x[0] * s[0] + x[1] * s[1] + x[2] * s[2]
            residual[lev, at : at + 8, :] = r[0] * s[0] + r[1] * s[1] + r[2] * s[2] + r[3] * s[3]


def shifted(x, axis, by):
    count = lax.axis_size(axis)
    return lax.ppermute(x, axis, [(i, i + by) for i in range(count) if 0 <= i + by < count])


def exchanged(cross, within):
    cross = over_chips(cross)
    within = on_chip(within)
    return cross, within


def over_chips(x):
    count = lax.axis_size(WIN)
    pairs = [(i, i + 1) for i in range(1, count - 1, 2)]
    return lax.ppermute(x, WIN, pairs + [(b, a) for a, b in pairs])


def on_chip(x):
    return lax.ppermute(x, "win_2", [(0, 1), (1, 0)])


def solve(right_side, error_weight, coeffs, obs_block, obs_pos, obs_weight):
    b, w, c = right_side[0], error_weight[0], coeffs[:, 0]
    levels, rows, width = b.shape
    total = rows + 2 * G
    field = shape(levels, total, width)
    fields = shape(4, levels, total, width)
    own = shape(levels, rows, width)
    ghost = shape(message_rows(levels), width)
    edges = shape(levels * EDGES, width)
    message = shape(levels, 40, width)

    north, south, b_e, c_e, w_e, d_e, cross_own, within_own = call(
        pack_kernel,
        [ghost, ghost, field, fields, field, field, own, own],
        hbm=True,
        count=6,
        scratch=(
            pltpu.VMEM(obs_pos.shape[1:], jnp.int32),
            pltpu.SMEM(obs_block.shape, jnp.int32),
            pltpu.VMEM(obs_weight.shape[1:], F32),
            pltpu.VMEM((b.size // 128, 128), F32),
            pltpu.SemaphoreType.DMA((6,)),
        ),
    )(*(in_hbm(x) for x in (b, c, w, obs_pos[0], obs_block, obs_weight[0])))
    from_south = shifted(north, "tile", -1)
    from_north = shifted(south, "tile", 1)
    cross_own = over_chips(cross_own)
    within_own = on_chip(within_own)
    w_next_own = shifted(w, WIN, -1)
    b_e, c_e, w_e, d_e, p0, cross, within = call(
        ghosts_kernel,
        [field, fields, field, field, field, edges, edges],
        aliases={2: 0, 3: 1, 4: 2, 5: 3},
        count=6,
    )(from_north, from_south, b_e, c_e, w_e, d_e)
    cross, within = exchanged(cross, within)
    scratch = (pltpu.VMEM((levels, total, width), F32),)
    q1, p1, w_next, cross, within, sums_1 = call(
        first_apply_kernel,
        [field, field, field, message, message, shape(3, 8, 128)],
        count=10,
        scratch=scratch * 3,
    )(b_e, c_e, w_e, d_e, p0, cross_own, within_own, w_next_own, cross, within)
    cross, within = exchanged(cross, within)
    q2, p2, cross, within, sums_2 = call(
        apply_kernel,
        [field, field, message, message, shape(2, 8, 128)],
        count=8,
        scratch=scratch,
    )(q1, c_e, w_e, d_e, p1, w_next, cross, within)
    cross, within = exchanged(cross, within)
    near, far = ("win_2", "tile"), ("win_0", "win_1")
    moments, q3 = call(
        moments_kernel, [shape(lax.axis_size(near), 8, 128), field], count=10, scratch=scratch
    )(q2, c_e, w_e, d_e, p2, w_next, cross, within, sums_1, sums_2)
    moments = lax.all_to_all(moments, near, 0, 0, tiled=True)
    (moments,) = call(spread_kernel, [shape(lax.axis_size(far), 8, 128)], count=1)(moments)
    moments = lax.all_to_all(moments, far, 0, 0, tiled=True)
    solution_field, residual = call(
        finish_kernel, [shape(levels, rows, width), shape(levels, rows, width)], count=5
    )(moments, b_e, q1, q2, q3)
    return solution_field[None], residual[None]


def solution(mesh):
    split = Mesh(
        mesh.devices.reshape(8, 8, 2, mesh.shape["tile"]), ("win_0", "win_1", "win_2", "tile")
    )
    in_specs = (
        P(WIN, None, "tile", None),
        P(WIN, None, "tile", None),
        P(None, WIN, None, "tile", None),
        P(WIN, "tile"),
        P(WIN, "tile", None),
        P(WIN, "tile", None),
    )
    out_specs = (P(WIN, None, "tile", None), P(WIN, None, "tile", None))
    return jax.shard_map(solve, mesh=split, in_specs=in_specs, out_specs=out_specs, check_vma=False)
```

```python
import jax
import jax.numpy as jnp
from jax import lax
from jax.experimental import pallas as pl
from jax.experimental.pallas import tpu as pltpu
from jax.sharding import Mesh
from jax.sharding import PartitionSpec as P


WIN = ("win_0", "win_1", "win_2")
THETA = 6.0
G = 8
F32 = jnp.float32


def call(body, out_shape, aliases=None, hbm=False, count=0, scratch=()):
    place = pltpu.HBM if hbm else pltpu.VMEM
    return pl.pallas_call(
        body,
        out_shape=out_shape,
        in_specs=[pl.BlockSpec(memory_space=place) for _ in range(count)],
        out_specs=[pl.BlockSpec(memory_space=pltpu.VMEM) for _ in out_shape],
        scratch_shapes=scratch,
        input_output_aliases=aliases or {},
        compiler_params=pltpu.CompilerParams(vmem_limit_bytes=24 * 2**20),
    )


def in_hbm(x):
    return pltpu.with_memory_space_constraint(x, pltpu.HBM)


def shape(*dims):
    return jax.ShapeDtypeStruct(dims, F32)


def west(x):
    return pltpu.roll(x, 1, axis=1)


def east(x):
    return pltpu.roll(x, x.shape[1] - 1, axis=1)


def north_of(ref, lev, tile):
    if tile == 0:
        return pltpu.roll(ref[lev, 0:8, :], 1, axis=0)
    return ref[lev, 8 * tile - 1 : 8 * tile + 7, :]


def south_of(ref, lev, tile, tiles):
    if tile == tiles - 1:
        return pltpu.roll(ref[lev, 8 * tile : 8 * tile + 8, :], 7, axis=0)
    return ref[lev, 8 * tile + 1 : 8 * tile + 9, :]


def folded(x):
    total = x[:, 0:128]
    for at in range(128, x.shape[1], 128):
        total = total + x[:, at : at + 128]
    return total


PARTS = (("b", 0, 5), ("c", 0, 4), ("c", 1, 5), ("c", 2, 4), ("c", 3, 4), ("w", 0, 5), ("d", 0, 4), ("p", 0, 1))
PER_LEVEL = sum(count for _, _, count in PARTS)
EDGES = 20


def ghost_items(levels):
    at = 0
    for lev in range(levels):
        for name, f, rows in PARTS:
            yield name, f, lev, at, rows
            at += rows


def pack_kernel(
    b_hbm, c_hbm, w_hbm, pos_hbm, block_hbm, weight_hbm,
    north, south, d_e,
    pos, block, weight, blocks, b, c, w, sems,
):
    levels, rows, width = b_hbm.shape
    per_row = width // 128
    pairs = [(pos_hbm, pos), (weight_hbm, weight), (block_hbm, block)]
    for side, first in enumerate((0, rows - 8)):
        edge = pl.ds(first, 8)
        pairs += [
            (b_hbm.at[:, edge, :], b.at[side]),
            (c_hbm.at[:, :, edge, :], c.at[side]),
            (w_hbm.at[:, edge, :], w.at[side]),
        ]
    moves = [pltpu.make_async_copy(src, dst, sems.at[i]) for i, (src, dst) in enumerate(pairs)]
    for move in moves:
        move.start()
    blank = jnp.zeros((G, width), F32)
    for lev in range(levels):
        d_e[lev, 0:G, :] = blank
        d_e[lev, G + rows :, :] = blank
    blocks[...] = jnp.zeros(blocks.shape, F32)
    for move in moves:
        move.wait()
    pos_all, weight_all = pos[...], weight[...]
    n = pos_all.shape[0]
    cell = lax.broadcasted_iota(jnp.int32, (n, 128), 1)
    sums = [jnp.zeros((n, 128), F32) for _ in range(4)]
    for j in range(pos_all.shape[1]):
        here = jnp.broadcast_to(pos_all[:, j : j + 1], (n, 128))
        value = jnp.broadcast_to(weight_all[:, j : j + 1], (n, 128))
        sums[j % 4] = sums[j % 4] + jnp.where(here == cell, value, 0.0)
    hot = (sums[0] + sums[1]) + (sums[2] + sums[3])
    for i in range(n):
        at = pl.ds(block[0, i], 1)
        blocks[at, :] = blocks[at, :] + hot[i : i + 1, :]
    for lev in range(levels):
        for j in range(per_row):
            first = lev * rows * per_row + j
            d_e[lev, G : G + rows, j * 128 : j * 128 + 128] = blocks[
                pl.ds(first, rows, stride=per_row), :
            ]
    for name, f, lev, at, count in ghost_items(levels):
        for side, out in enumerate((north, south)):
            own = 0 if side == 0 else 8 - count
            if name == "p":
                image = model_tile(b.at[side], c.at[side], lev, 0, 1)
                piece = image[4:5, :] if side == 0 else image[3:4, :]
            elif name == "d":
                own = G if side == 0 else G + rows - count
                piece = d_e[lev, own : own + count, :]
            elif name == "c":
                piece = c[side, f, lev, own : own + count, :]
            else:
                piece = (b if name == "b" else w)[side, lev, own : own + count, :]
            out[at : at + count, :] = piece


def extend_kernel(b, c, w, b_e, c_e, w_e, cross, within):
    levels, rows, width = b.shape
    blank = jnp.zeros((G, width), F32)
    for lev in range(levels):
        targets = [(b_e.at[lev], b.at[lev]), (w_e.at[lev], w.at[lev])]
        targets += [(c_e.at[f, lev], c.at[f, lev]) for f in range(4)]
        for out, src in targets:
            out[0:G, :] = blank
            out[G : G + rows, :] = src[...]
            out[G + rows :, :] = blank

    def send(forward, backward):
        for lev in range(levels):
            backward[lev, :, :] = b[lev, :, :]
            for tile in range(rows // 8):
                forward[lev, 8 * tile : 8 * tile + 8, :] = model_tile(b, c, lev, tile, rows // 8)

    @pl.when(core_is_one())
    def _():
        send(cross, within)

    @pl.when(jnp.logical_not(core_is_one()))
    def _():
        send(within, cross)


def model_tile(q, c, lev, tile, tiles):
    here = q[lev, 8 * tile : 8 * tile + 8, :]
    at = slice(8 * tile, 8 * tile + 8)
    return (
        c[0, lev, at, :] * here
        + c[1, lev, at, :] * (north_of(q, lev, tile) + south_of(q, lev, tile, tiles))
        + c[2, lev, at, :] * east(here)
        + c[3, lev, at, :] * west(here)
    )


def propagate(q, c, p):
    levels, rows, _ = q.shape
    for lev in range(levels):
        for tile in range(rows // 8):
            p[lev, 8 * tile : 8 * tile + 8, :] = model_tile(q, c, lev, tile, rows // 8)


def post(out, values, lev):
    reach = out.shape[1] - (values.shape[1] - 2 * G)
    first = G - reach // 2
    out[lev, :, :] = values[lev, first : first + out.shape[1], :]


def core_is_one():
    return lax.axis_index("win_2") == 1


def ghosts_kernel(from_north, from_south, b_in, c_in, w_in, d_in, b_e, c_e, w_e, d_e, p, cross, within):
    levels, total, width = b_e.shape
    rows = total - 2 * G

    def fill(names):
        for name, f, lev, at, count in ghost_items(levels):
            if name in names:
                out = {"b": b_e, "c": c_e.at[f], "w": w_e, "d": d_e, "p": p}[name]
                reach = 5 if name == "p" else count
                low, high = G - reach, G + rows + reach - count
                out[lev, low : low + count, :] = from_north[at : at + count, :]
                out[lev, high : high + count, :] = from_south[at : at + count, :]

    fill("bcwd")
    propagate(b_e, c_e, p)
    fill("p")

    def send(forward, backward):
        for lev in range(levels):
            at = lev * EDGES
            for f, (field, first) in enumerate(((b_e, 3), (w_e, 3))):
                low, high = at + 10 * f, at + 10 * f + 5
                backward[low : low + 5, :] = field[lev, first : first + 5, :]
                backward[high : high + 5, :] = field[lev, G + rows : G + rows + 5, :]
            forward[at : at + 5, :] = p[lev, 4:9, :]
            forward[at + 5 : at + 10, :] = p[lev, G + rows - 1 : G + rows + 4, :]
            forward[at + 10 : at + EDGES, :] = jnp.zeros((EDGES - 10, width), F32)

    @pl.when(core_is_one())
    def _():
        send(cross, within)

    @pl.when(jnp.logical_not(core_is_one()))
    def _():
        send(within, cross)


def unposted(ref, lev, tile, tiles):
    if tile == 0:
        return pltpu.roll(ref[lev, 0:8, :], 4, axis=0)
    if tile == tiles - 1:
        return pltpu.roll(ref[lev, 8 * tile - 8 : 8 * tile, :], 4, axis=0)
    return ref[lev, 8 * tile - 4 : 8 * tile + 4, :]


def second_half(q, c, w, d, p, v_next, w_next, p_prev, out, edge):
    levels, total, _ = q.shape
    tiles = total // 8
    for lev in range(levels):
        for tile in range(tiles):
            at = slice(8 * tile, 8 * tile + 8)
            here, weight = q[lev, at, :], w[lev, at, :]
            following = w_next(lev, tile) * (v_next(lev, tile) - p[lev, at, :])
            edge[lev, at, :] = c[1, lev, at, :] * following
            out[lev, at, :] = (
                (weight + d[lev, at, :] - THETA) * here
                - weight * p_prev(lev, tile)
                - c[0, lev, at, :] * following
                - west(c[2, lev, at, :] * following)
                - east(c[3, lev, at, :] * following)
            )
    for lev in range(levels):
        for tile in range(tiles):
            at = slice(8 * tile, 8 * tile + 8)
            value = out[lev, at, :] - (north_of(edge, lev, tile) + south_of(edge, lev, tile, tiles))
            if tile in (0, tiles - 1):
                value = jnp.where(w[lev, at, :] > 0.0, value, 0.0)
            out[lev, at, :] = value


def products_kernel(x, y, out):
    levels, total, _ = x.shape
    totals = [jnp.zeros((8, 128), F32) for _ in range(out.shape[0])]
    for lev in range(levels):
        for at in range(G, total - G, 8):
            u, v = x[lev, at : at + 8, :], y[lev, at : at + 8, :]
            for i, (a, b) in enumerate(((u, v), (v, v), (u, u))[: len(totals)]):
                totals[i] = totals[i] + folded(a * b)
    for i, part in enumerate(totals):
        out[i] = part


def send_both(q, p, cross, within):
    def send(forward, backward):
        for lev in range(q.shape[0]):
            post(forward, p, lev)
            post(backward, q, lev)

    @pl.when(core_is_one())
    def _():
        send(cross, within)

    @pl.when(jnp.logical_not(core_is_one()))
    def _():
        send(within, cross)


def first_apply_kernel(
    b_e, c, w, d, p0, cross_own, within_own, w_next_own, cross_in, within_in,
    q1, p1, w_next, cross, within, edge, v_next, p_prev,
):
    levels, total, width = b_e.shape
    rows = total - 2 * G

    def assemble(p_own, v_own, p_edges, v_edges):
        for lev in range(levels):
            at = lev * EDGES
            for out, src in ((p_prev, p_own), (v_next, v_own), (w_next, w_next_own)):
                out[lev, G : G + rows, :] = src[lev, :, :]
            for f, out in enumerate((v_next, w_next)):
                low, high = at + 10 * f, at + 10 * f + 5
                out[lev, 3:8, :] = v_edges[low : low + 5, :]
                out[lev, G + rows : G + rows + 5, :] = v_edges[high : high + 5, :]
            p_prev[lev, 4:9, :] = p_edges[at : at + 5, :]
            p_prev[lev, G + rows - 1 : G + rows + 4, :] = p_edges[at + 5 : at + 10, :]

    blank = jnp.zeros((G, width), F32)
    for lev in range(levels):
        for out in (p_prev, v_next, w_next):
            out[lev, 0:G, :] = blank
            out[lev, G + rows :, :] = blank

    @pl.when(core_is_one())
    def _():
        assemble(within_own, cross_own, within_in, cross_in)

    @pl.when(jnp.logical_not(core_is_one()))
    def _():
        assemble(cross_own, within_own, cross_in, within_in)

    def tile_of(ref):
        return lambda lev, tile: ref[lev, 8 * tile : 8 * tile + 8, :]

    second_half(
        b_e, c, w, d, p0, tile_of(v_next), tile_of(w_next), tile_of(p_prev), q1, edge
    )
    propagate(q1, c, p1)
    send_both(q1, p1, cross, within)


def apply_kernel(
    q1, c, w, d, p1, w_next, cross_in, within_in, q2, p2, cross, within, edge
):
    _, total, _ = q1.shape
    tiles = total // 8
    one = core_is_one()

    def v_next(lev, tile):
        return jnp.where(
            one, unposted(cross_in, lev, tile, tiles), unposted(within_in, lev, tile, tiles)
        )

    def p_prev(lev, tile):
        return jnp.where(
            one, unposted(within_in, lev, tile, tiles), unposted(cross_in, lev, tile, tiles)
        )

    second_half(
        q1, c, w, d, p1, v_next,
        lambda lev, tile: w_next[lev, 8 * tile : 8 * tile + 8, :], p_prev, q2, edge,
    )
    propagate(q2, c, p2)
    send_both(q2, p2, cross, within)


def moments_kernel(q2, c, w, d, p2, w_next, cross_in, within_in, sums_1, sums_2, out, q3, edge, v_next, p_prev):
    levels, total, _ = q2.shape
    tiles = total // 8
    one = core_is_one()
    first = jnp.logical_and(
        lax.axis_index("win_0") + lax.axis_index("win_1") == 0, jnp.logical_not(one)
    )

    @pl.when(one)
    def _():
        v_next[...] = cross_in[...]
        p_prev[...] = within_in[...]

    @pl.when(jnp.logical_not(one))
    def _():
        v_next[...] = within_in[...]
        p_prev[...] = cross_in[...]

    last = jnp.zeros((8, 128), F32)
    for lev in range(levels):
        for tile in range(1, tiles - 1):
            at = slice(8 * tile, 8 * tile + 8)
            here, weight = q2[lev, at, :], w[lev, at, :]
            gap = v_next[lev, 8 * tile - 4 : 8 * tile + 4, :] - p2[lev, at, :]
            following = w_next[lev, at, :] * gap
            diagonal = d[lev, at, :] - THETA
            own = diagonal + jnp.where(first, weight, 0.0)
            last = last + folded(following * gap + own * here * here)
            edge[lev, at, :] = c[1, lev, at, :] * following
            q3[lev, at, :] = (
                (weight + diagonal) * here
                - weight * p_prev[lev, 8 * tile - 4 : 8 * tile + 4, :]
                - c[0, lev, at, :] * following
                - west(c[2, lev, at, :] * following)
                - east(c[3, lev, at, :] * following)
            )
        for row, at in ((G - 1, 3), (total - G, total - G - 4)):
            following = w_next[lev, row : row + 1, :] * (
                v_next[lev, at : at + 1, :] - p2[lev, row : row + 1, :]
            )
            edge[lev, row : row + 1, :] = c[1, lev, row : row + 1, :] * following
        for tile in range(1, tiles - 1):
            at = slice(8 * tile, 8 * tile + 8)
            q3[lev, at, :] = q3[lev, at, :] - (
                north_of(edge, lev, tile) + south_of(edge, lev, tile, tiles)
            )
    lane = lax.broadcasted_iota(jnp.int32, (1, 128), 1)
    result = jnp.zeros((1, 128), F32)
    parts = [sums_1[2], sums_1[0], sums_1[1], sums_2[0], sums_2[1], last]
    for i, part in enumerate(parts):
        total_i = jnp.sum(jnp.sum(part, axis=0, keepdims=True), axis=1, keepdims=True)
        result = jnp.where(lane == i, jnp.broadcast_to(total_i, (1, 128)), result)
    for i in range(out.shape[0]):
        out[i] = result


def spread_kernel(x, out):
    total = summed(x)
    for i in range(out.shape[0]):
        out[i] = total


def summed(x):
    parts = [x[i] for i in range(x.shape[0])]
    while len(parts) > 1:
        parts = [a + b for a, b in zip(parts[::2], parts[1::2])]
    return parts[0]


def times_a(v):
    longer = [THETA * x for x in v] + [0.0]
    return [longer[i] + (v[i - 1] if i else 0.0) for i in range(len(longer))]


def inner(u, v, mu):
    return sum(x * y * mu[i + j] for i, x in enumerate(u) for j, y in enumerate(v))


def plus(u, scale, v):
    size = max(len(u), len(v))
    u, v = u + [0.0] * (size - len(u)), v + [0.0] * (size - len(v))
    return [x + scale * y for x, y in zip(u, v)]


def coordinates(mu, iters=3):
    x, r, p = [0.0], [1.0], [1.0]
    rr = mu[0]
    for i in range(iters):
        image = times_a(p)
        alpha = rr / inner(p, image, mu)
        x = plus(x, alpha, p)
        r = plus(r, -alpha, image)
        if i + 1 < iters:
            new = inner(r, r, mu)
            p = plus(r, new / rr, p)
            rr = new
    return x, r


def finish_kernel(parts, q0, q1, q2, q3, solution_field, residual):
    levels, rows, width = solution_field.shape
    total = summed(parts)
    mu = [jnp.broadcast_to(total[:, i : i + 1], (8, 128)) for i in range(6)]
    x, r = coordinates(mu)
    wide = lambda v: jnp.concatenate([v] * (width // 128), axis=1)
    x = [wide(v) for v in x]
    r = [wide(v) for v in r]
    for lev in range(levels):
        for at in range(0, rows, 8):
            s = [q[lev, G + at : G + at + 8, :] for q in (q0, q1, q2, q3)]
            solution_field[lev, at : at + 8, :] = x[0] * s[0] + x[1] * s[1] + x[2] * s[2]
            residual[lev, at : at + 8, :] = r[0] * s[0] + r[1] * s[1] + r[2] * s[2] + r[3] * s[3]


def shifted(x, axis, by):
    count = lax.axis_size(axis)
    return lax.ppermute(x, axis, [(i, i + by) for i in range(count) if 0 <= i + by < count])


def exchanged(cross, within):
    cross = over_chips(cross)
    within = on_chip(within)
    return cross, within


def over_chips(x):
    count = lax.axis_size(WIN)
    pairs = [(i, i + 1) for i in range(1, count - 1, 2)]
    return lax.ppermute(x, WIN, pairs + [(b, a) for a, b in pairs])


def on_chip(x):
    return lax.ppermute(x, "win_2", [(0, 1), (1, 0)])


def solve(right_side, error_weight, coeffs, obs_block, obs_pos, obs_weight):
    b, w, c = right_side[0], error_weight[0], coeffs[:, 0]
    levels, rows, width = b.shape
    total = rows + 2 * G
    field = shape(levels, total, width)
    fields = shape(4, levels, total, width)
    own = shape(levels, rows, width)
    ghost = shape(levels * PER_LEVEL, width)
    edges = shape(levels * EDGES, width)
    message = shape(levels, rows + 8, width)
    scratch = pltpu.VMEM((levels, total, width), F32)

    north, south, d_e = call(
        pack_kernel,
        [ghost, ghost, field],
        hbm=True,
        count=6,
        scratch=(
            pltpu.VMEM(obs_pos.shape[1:], jnp.int32),
            pltpu.SMEM(obs_block.shape, jnp.int32),
            pltpu.VMEM(obs_weight.shape[1:], F32),
            pltpu.VMEM((b.size // 128, 128), F32),
            pltpu.VMEM((2, levels, 8, width), F32),
            pltpu.VMEM((2, 4, levels, 8, width), F32),
            pltpu.VMEM((2, levels, 8, width), F32),
            pltpu.SemaphoreType.DMA((9,)),
        ),
    )(*(in_hbm(x) for x in (b, c, w, obs_pos[0], obs_block, obs_weight[0])))
    from_south = shifted(north, "tile", -1)
    from_north = shifted(south, "tile", 1)
    b_e, c_e, w_e, cross_own, within_own = call(
        extend_kernel, [field, fields, field, own, own], count=3
    )(b, c, w)
    cross_own = over_chips(cross_own)
    within_own = on_chip(within_own)
    w_next_own = shifted(w, WIN, -1)
    b_e, c_e, w_e, d_e, p0, cross, within = call(
        ghosts_kernel,
        [field, fields, field, field, field, edges, edges],
        aliases={2: 0, 3: 1, 4: 2, 5: 3},
        count=6,
    )(from_north, from_south, b_e, c_e, w_e, d_e)
    cross, within = exchanged(cross, within)
    q1, p1, w_next, cross, within = call(
        first_apply_kernel,
        [field, field, field, message, message],
        count=10,
        scratch=(scratch,) * 3,
    )(b_e, c_e, w_e, d_e, p0, cross_own, within_own, w_next_own, cross, within)
    cross, within = exchanged(cross, within)
    (sums_1,) = call(products_kernel, [shape(3, 8, 128)], count=2)(b_e, q1)
    q2, p2, cross, within = call(
        apply_kernel, [field, field, message, message], count=8, scratch=(scratch,)
    )(q1, c_e, w_e, d_e, p1, w_next, cross, within)
    cross, within = exchanged(cross, within)
    (sums_2,) = call(products_kernel, [shape(2, 8, 128)], count=2)(q1, q2)
    near, far = ("win_1", "tile"), ("win_0", "win_2")
    moments, q3 = call(
        moments_kernel,
        [shape(lax.axis_size(near), 1, 128), field],
        count=10,
        scratch=(scratch,) + (pltpu.VMEM((levels, rows + 8, width), F32),) * 2,
    )(q2, c_e, w_e, d_e, p2, w_next, cross, within, sums_1, sums_2)
    moments = lax.all_to_all(moments, near, 0, 0, tiled=True)
    (moments,) = call(spread_kernel, [shape(lax.axis_size(far), 1, 128)], count=1)(moments)
    moments = lax.all_to_all(moments, far, 0, 0, tiled=True)
    solution_field, residual = call(finish_kernel, [own, own], count=5)(moments, b_e, q1, q2, q3)
    return solution_field[None], residual[None]


def solution(mesh):
    split = Mesh(
        mesh.devices.reshape(8, 8, 2, mesh.shape["tile"]), ("win_0", "win_1", "win_2", "tile")
    )
    in_specs = (
        P(WIN, None, "tile", None),
        P(WIN, None, "tile", None),
        P(None, WIN, None, "tile", None),
        P(WIN, "tile"),
        P(WIN, "tile", None),
        P(WIN, "tile", None),
    )
    out_specs = (P(WIN, None, "tile", None), P(WIN, None, "tile", None))
    return jax.shard_map(solve, mesh=split, in_specs=in_specs, out_specs=out_specs, check_vma=False)
```

```python
import jax
import jax.numpy as jnp
from jax import lax
from jax.experimental import pallas as pl
from jax.experimental.pallas import tpu as pltpu
from jax.sharding import Mesh
from jax.sharding import PartitionSpec as P


WIN = ("win_0", "win_1", "win_2")
THETA = 6.0
G = 8
F32 = jnp.float32


def call(body, out_shape, aliases=None, hbm=False, count=0, scratch=()):
    place = pltpu.HBM if hbm else pltpu.VMEM
    return pl.pallas_call(
        body,
        out_shape=out_shape,
        in_specs=[pl.BlockSpec(memory_space=place) for _ in range(count)],
        out_specs=[pl.BlockSpec(memory_space=pltpu.VMEM) for _ in out_shape],
        scratch_shapes=scratch,
        input_output_aliases=aliases or {},
        compiler_params=pltpu.CompilerParams(vmem_limit_bytes=24 * 2**20),
    )


def in_hbm(x):
    return pltpu.with_memory_space_constraint(x, pltpu.HBM)


def shape(*dims):
    return jax.ShapeDtypeStruct(dims, F32)


def west(x):
    return pltpu.roll(x, 1, axis=1)


def east(x):
    return pltpu.roll(x, x.shape[1] - 1, axis=1)


def north_of(ref, lev, tile):
    if tile == 0:
        return pltpu.roll(ref[lev, 0:8, :], 1, axis=0)
    return ref[lev, 8 * tile - 1 : 8 * tile + 7, :]


def south_of(ref, lev, tile, tiles):
    if tile == tiles - 1:
        return pltpu.roll(ref[lev, 8 * tile : 8 * tile + 8, :], 7, axis=0)
    return ref[lev, 8 * tile + 1 : 8 * tile + 9, :]


def folded(x):
    total = x[:, 0:128]
    for at in range(128, x.shape[1], 128):
        total = total + x[:, at : at + 128]
    return total


PARTS = (("b", 0, 5), ("c", 0, 4), ("c", 1, 5), ("c", 2, 4), ("c", 3, 4), ("w", 0, 5), ("d", 0, 4), ("p", 0, 1))
PER_LEVEL = sum(count for _, _, count in PARTS)
EDGES = 20


def ghost_items(levels):
    at = 0
    for lev in range(levels):
        for name, f, rows in PARTS:
            yield name, f, lev, at, rows
            at += rows


def pack_kernel(
    b_hbm, c_hbm, w_hbm, pos_hbm, block_hbm, weight_hbm,
    first, second, b_e, c_e, w_e, d_e,
    pos, block, weight, blocks, sems,
):
    levels, rows, width = b_hbm.shape
    per_row = width // 128
    own = pl.ds(G, rows)
    pairs = (
        (pos_hbm, pos),
        (weight_hbm, weight),
        (block_hbm, block),
        (b_hbm, b_e.at[:, own, :]),
        (w_hbm, w_e.at[:, own, :]),
        (c_hbm, c_e.at[:, :, own, :]),
    )
    moves = [pltpu.make_async_copy(src, dst, sems.at[i]) for i, (src, dst) in enumerate(pairs)]
    for move in moves:
        move.start()
    blank = jnp.zeros((G, width), F32)
    for lev in range(levels):
        for out in (b_e.at[lev], w_e.at[lev], d_e.at[lev], *(c_e.at[f, lev] for f in range(4))):
            out[0:G, :] = blank
            out[G + rows :, :] = blank
    blocks[...] = jnp.zeros(blocks.shape, F32)
    for move in moves[:3]:
        move.wait()
    hot = block_sums(pos[...].astype(F32), weight[...])
    for i in range(hot.shape[0]):
        at = pl.ds(block[0, i], 1)
        blocks[at, :] = blocks[at, :] + hot[i : i + 1, :]
    for lev in range(levels):
        for j in range(per_row):
            start = lev * rows * per_row + j
            d_e[lev, G : G + rows, j * 128 : j * 128 + 128] = blocks[
                pl.ds(start, rows, stride=per_row), :
            ]
    for move in moves[3:]:
        move.wait()

    def fill(north, south):
        for name, f, lev, at, count in ghost_items(levels):
            for out, start in ((north, G), (south, G + rows - count)):
                if name == "p":
                    tile = 1 if out is north else rows // 8
                    image = model_tile(b_e, c_e, lev, tile, 2 + rows // 8)
                    piece = image[4:5, :] if out is north else image[3:4, :]
                else:
                    src = {"b": b_e, "c": c_e.at[f], "w": w_e, "d": d_e}[name]
                    piece = src[lev, start : start + count, :]
                out[at : at + count, :] = piece

    by_parity(lambda: fill(second, first), lambda: fill(first, second))


def by_parity(even, odd):
    is_even = lax.axis_index("tile") % 2 == 0
    pl.when(is_even)(even)
    pl.when(jnp.logical_not(is_even))(odd)


def block_sums(pos, weight):
    n, width = pos.shape
    groups = width // n

    def packed(x):
        turned = x.T
        return jnp.concatenate([turned[g * n : g * n + n, :] for g in range(groups)], axis=1)

    pos, weight = packed(pos), packed(weight)
    cell = lax.broadcasted_iota(jnp.int32, (width, width), 0).astype(F32)
    total = jnp.zeros((width, width), F32)
    for i in range(n):
        here = jnp.broadcast_to(pos[i : i + 1, :], (width, width))
        value = jnp.broadcast_to(weight[i : i + 1, :], (width, width))
        total = total + jnp.where(here == cell, value, 0.0)
    shift = width // 2
    while shift >= n:
        total = total + pltpu.roll(total, shift, axis=1)
        shift //= 2
    return total.T[0:n, :]


def extend_kernel(b_e, c_e, cross):
    levels, total, _ = b_e.shape
    rows = total - 2 * G

    @pl.when(core_is_one())
    def _():
        for lev in range(levels):
            for tile in range(1, 1 + rows // 8):
                at = 8 * tile - G
                cross[lev, at : at + 8, :] = model_tile(b_e, c_e, lev, tile, 2 + rows // 8)

    @pl.when(jnp.logical_not(core_is_one()))
    def _():
        for lev in range(levels):
            cross[lev, :, :] = b_e[lev, G : G + rows, :]


def model_tile(q, c, lev, tile, tiles):
    here = q[lev, 8 * tile : 8 * tile + 8, :]
    at = slice(8 * tile, 8 * tile + 8)
    return (
        c[0, lev, at, :] * here
        + c[1, lev, at, :] * (north_of(q, lev, tile) + south_of(q, lev, tile, tiles))
        + c[2, lev, at, :] * east(here)
        + c[3, lev, at, :] * west(here)
    )


def propagate(q, c, p):
    levels, rows, _ = q.shape
    for lev in range(levels):
        for tile in range(rows // 8):
            p[lev, 8 * tile : 8 * tile + 8, :] = model_tile(q, c, lev, tile, rows // 8)


def post(out, values, lev):
    if len(out.shape) == 2:
        rows = values.shape[1] - 2 * G + 2
        out[lev * rows : lev * rows + rows, :] = values[lev, G - 1 : G - 1 + rows, :]
    else:
        out[lev, :, :] = values[lev, 4 : 4 + out.shape[1], :]


def core_is_one():
    return lax.axis_index("win_2") == 1


def ghosts_kernel(first, second, b_in, c_in, w_in, d_in, b_e, c_e, w_e, d_e, p, cross, within):
    levels, total, width = b_e.shape
    rows = total - 2 * G

    def fill(names, from_north, from_south):
        for name, f, lev, at, count in ghost_items(levels):
            if name in names:
                out = {"b": b_e, "c": c_e.at[f], "w": w_e, "d": d_e, "p": p}[name]
                reach = 5 if name == "p" else count
                low, high = G - reach, G + rows + reach - count
                out[lev, low : low + count, :] = from_north[at : at + count, :]
                out[lev, high : high + count, :] = from_south[at : at + count, :]

    by_parity(lambda: fill("bcwd", second, first), lambda: fill("bcwd", first, second))
    propagate(b_e, c_e, p)
    by_parity(lambda: fill("p", second, first), lambda: fill("p", first, second))

    @pl.when(core_is_one())
    def _():
        for lev in range(levels):
            at = lev * EDGES
            cross[at : at + 5, :] = p[lev, 4:9, :]
            cross[at + 5 : at + 10, :] = p[lev, G + rows - 1 : G + rows + 4, :]
            cross[at + 10 : at + EDGES, :] = jnp.zeros((EDGES - 10, width), F32)
            within[lev] = b_e[lev]
            within[levels + lev] = w_e[lev]

    @pl.when(jnp.logical_not(core_is_one()))
    def _():
        for lev in range(levels):
            for f, field in enumerate((b_e, w_e)):
                low, high = lev * EDGES + 10 * f, lev * EDGES + 10 * f + 5
                cross[low : low + 5, :] = field[lev, 3:8, :]
                cross[high : high + 5, :] = field[lev, G + rows : G + rows + 5, :]
            within[lev] = p[lev]
            within[levels + lev] = p[lev]


def unposted(ref, lev, tile, tiles):
    if tile == 0:
        return pltpu.roll(ref[lev, 0:8, :], 4, axis=0)
    if tile == tiles - 1:
        return pltpu.roll(ref[lev, 8 * tile - 8 : 8 * tile, :], 4, axis=0)
    return ref[lev, 8 * tile - 4 : 8 * tile + 4, :]


def second_half(q, c, w, d, p, v_next, w_next, p_prev, out, edge):
    levels, total, _ = q.shape
    tiles = total // 8
    for lev in range(levels):
        for tile in range(tiles):
            at = slice(8 * tile, 8 * tile + 8)
            here, weight = q[lev, at, :], w[lev, at, :]
            following = w_next(lev, tile) * (v_next(lev, tile) - p[lev, at, :])
            edge[lev, at, :] = c[1, lev, at, :] * following
            out[lev, at, :] = (
                (weight + d[lev, at, :] - THETA) * here
                - weight * p_prev(lev, tile)
                - c[0, lev, at, :] * following
                - west(c[2, lev, at, :] * following)
                - east(c[3, lev, at, :] * following)
            )
    for lev in range(levels):
        for tile in range(tiles):
            at = slice(8 * tile, 8 * tile + 8)
            value = out[lev, at, :] - (north_of(edge, lev, tile) + south_of(edge, lev, tile, tiles))
            if tile in (0, tiles - 1):
                value = jnp.where(w[lev, at, :] > 0.0, value, 0.0)
            out[lev, at, :] = value


def products_kernel(x, y, out):
    levels, total, _ = x.shape
    totals = [jnp.zeros((8, 128), F32) for _ in range(out.shape[0])]
    for lev in range(levels):
        for at in range(G, total - G, 8):
            u, v = x[lev, at : at + 8, :], y[lev, at : at + 8, :]
            for i, (a, b) in enumerate(((u, v), (v, v), (u, u))[: len(totals)]):
                totals[i] = totals[i] + folded(a * b)
    for i, part in enumerate(totals):
        out[i] = part


def send_both(q, p, cross, within):
    def send(forward, backward):
        for lev in range(q.shape[0]):
            post(forward, p, lev)
            post(backward, q, lev)

    @pl.when(core_is_one())
    def _():
        send(cross, within)

    @pl.when(jnp.logical_not(core_is_one()))
    def _():
        send(within, cross)


def first_apply_kernel(
    b_e, c, w, d, p0, cross_own, w_next_own, cross_in, within_in,
    q1, p1, w_next, cross, within, edge, v_next, p_prev,
):
    levels, total, width = b_e.shape
    rows = total - 2 * G
    blank = jnp.zeros((G, width), F32)

    @pl.when(core_is_one())
    def _():
        for lev in range(levels):
            p_prev[lev] = within_in[lev]
            for f, (out, src) in enumerate(((v_next, cross_own), (w_next, w_next_own))):
                low, high = lev * EDGES + 10 * f, lev * EDGES + 10 * f + 5
                out[lev, 0:G, :] = blank
                out[lev, G : G + rows, :] = src[lev]
                out[lev, G + rows :, :] = blank
                out[lev, 3:8, :] = cross_in[low : low + 5, :]
                out[lev, G + rows : G + rows + 5, :] = cross_in[high : high + 5, :]

    @pl.when(jnp.logical_not(core_is_one()))
    def _():
        for lev in range(levels):
            at = lev * EDGES
            v_next[lev] = within_in[lev]
            w_next[lev] = within_in[levels + lev]
            p_prev[lev, 0:G, :] = blank
            p_prev[lev, G : G + rows, :] = cross_own[lev]
            p_prev[lev, G + rows :, :] = blank
            p_prev[lev, 4:9, :] = cross_in[at : at + 5, :]
            p_prev[lev, G + rows - 1 : G + rows + 4, :] = cross_in[at + 5 : at + 10, :]

    def tile_of(ref):
        return lambda lev, tile: ref[lev, 8 * tile : 8 * tile + 8, :]

    second_half(
        b_e, c, w, d, p0, tile_of(v_next), tile_of(w_next), tile_of(p_prev), q1, edge
    )
    propagate(q1, c, p1)
    send_both(q1, p1, cross, within)


def apply_kernel(
    q1, c, w, d, p1, w_next, cross_in, within_in, q2, p2, cross, within, edge
):
    _, total, _ = q1.shape
    tiles = total // 8
    one = core_is_one()

    def v_next(lev, tile):
        return jnp.where(
            one, unposted(cross_in, lev, tile, tiles), unposted(within_in, lev, tile, tiles)
        )

    def p_prev(lev, tile):
        return jnp.where(
            one, unposted(within_in, lev, tile, tiles), unposted(cross_in, lev, tile, tiles)
        )

    second_half(
        q1, c, w, d, p1, v_next,
        lambda lev, tile: w_next[lev, 8 * tile : 8 * tile + 8, :], p_prev, q2, edge,
    )
    propagate(q2, c, p2)
    send_both(q2, p2, cross, within)


def moments_kernel(q2, c, w, d, p2, w_next, cross_in, within_in, sums_1, sums_2, out, q3, edge, v_next, p_prev):
    levels, total, _ = q2.shape
    tiles = total // 8
    one = core_is_one()
    opening = jnp.logical_and(
        lax.axis_index("win_0") + lax.axis_index("win_1") == 0, jnp.logical_not(one)
    )

    @pl.when(one)
    def _():
        v_next[...] = cross_in[...]
        p_prev[...] = within_in[...]

    @pl.when(jnp.logical_not(one))
    def _():
        v_next[...] = within_in[...]
        p_prev[...] = cross_in[...]

    last = jnp.zeros((8, 128), F32)
    for lev in range(levels):
        base = lev * (total - 2 * G + 2)
        for tile in range(1, tiles - 1):
            at = slice(8 * tile, 8 * tile + 8)
            here, weight = q2[lev, at, :], w[lev, at, :]
            got = slice(base + 8 * tile - G + 1, base + 8 * tile - G + 9)
            gap = v_next[got, :] - p2[lev, at, :]
            following = w_next[lev, at, :] * gap
            diagonal = d[lev, at, :] - THETA
            own = diagonal + jnp.where(opening, weight, 0.0)
            last = last + folded(following * gap + own * here * here)
            edge[lev, at, :] = c[1, lev, at, :] * following
            q3[lev, at, :] = (
                (weight + diagonal) * here
                - weight * p_prev[got, :]
                - c[0, lev, at, :] * following
                - west(c[2, lev, at, :] * following)
                - east(c[3, lev, at, :] * following)
            )
        for row, at in ((G - 1, base), (total - G, base + total - 2 * G + 1)):
            following = w_next[lev, row : row + 1, :] * (
                v_next[at : at + 1, :] - p2[lev, row : row + 1, :]
            )
            edge[lev, row : row + 1, :] = c[1, lev, row : row + 1, :] * following
        for tile in range(1, tiles - 1):
            at = slice(8 * tile, 8 * tile + 8)
            q3[lev, at, :] = q3[lev, at, :] - (
                north_of(edge, lev, tile) + south_of(edge, lev, tile, tiles)
            )
    lane = lax.broadcasted_iota(jnp.int32, (1, 128), 1)
    result = jnp.zeros((1, 128), F32)
    parts = [sums_1[2], sums_1[0], sums_1[1], sums_2[0], sums_2[1], last]
    for i, part in enumerate(parts):
        total_i = jnp.sum(jnp.sum(part, axis=0, keepdims=True), axis=1, keepdims=True)
        result = jnp.where(lane == i, jnp.broadcast_to(total_i, (1, 128)), result)
    for i in range(out.shape[0]):
        out[i] = result


def spread_kernel(x, out):
    total = summed(x)
    for i in range(out.shape[0]):
        out[i] = total


def summed(x):
    parts = [x[i] for i in range(x.shape[0])]
    while len(parts) > 1:
        parts = [a + b for a, b in zip(parts[::2], parts[1::2])]
    return parts[0]


def times_a(v):
    longer = [THETA * x for x in v] + [0.0]
    return [longer[i] + (v[i - 1] if i else 0.0) for i in range(len(longer))]


def inner(u, v, mu):
    return sum(x * y * mu[i + j] for i, x in enumerate(u) for j, y in enumerate(v))


def plus(u, scale, v):
    size = max(len(u), len(v))
    u, v = u + [0.0] * (size - len(u)), v + [0.0] * (size - len(v))
    return [x + scale * y for x, y in zip(u, v)]


def coordinates(mu, iters=3):
    x, r, p = [0.0], [1.0], [1.0]
    rr = mu[0]
    for i in range(iters):
        image = times_a(p)
        alpha = rr / inner(p, image, mu)
        x = plus(x, alpha, p)
        r = plus(r, -alpha, image)
        if i + 1 < iters:
            new = inner(r, r, mu)
            p = plus(r, new / rr, p)
            rr = new
    return x, r


def finish_kernel(parts, q0, q1, q2, q3, solution_field, residual):
    levels, rows, width = solution_field.shape
    total = summed(parts)
    mu = [jnp.broadcast_to(total[:, i : i + 1], (8, 128)) for i in range(6)]
    x, r = coordinates(mu)
    wide = lambda v: jnp.concatenate([v] * (width // 128), axis=1)
    x = [wide(v) for v in x]
    r = [wide(v) for v in r]
    for lev in range(levels):
        for at in range(0, rows, 8):
            s = [q[lev, G + at : G + at + 8, :] for q in (q0, q1, q2, q3)]
            solution_field[lev, at : at + 8, :] = x[0] * s[0] + x[1] * s[1] + x[2] * s[2]
            residual[lev, at : at + 8, :] = r[0] * s[0] + r[1] * s[1] + r[2] * s[2] + r[3] * s[3]


def swapped(x, axis, start):
    pairs = [(i, i + 1) for i in range(start, lax.axis_size(axis) - 1, 2)]
    return lax.ppermute(x, axis, pairs + [(b, a) for a, b in pairs])


def exchanged(cross, within):
    cross = over_chips(cross)
    within = on_chip(within)
    return cross, within


def over_chips(x):
    return swapped(x, WIN, 1)


def on_chip(x):
    return lax.ppermute(x, "win_2", [(0, 1), (1, 0)])


def solve(right_side, error_weight, coeffs, obs_block, obs_pos, obs_weight):
    b, w, c = right_side[0], error_weight[0], coeffs[:, 0]
    levels, rows, width = b.shape
    total = rows + 2 * G
    field = shape(levels, total, width)
    fields = shape(4, levels, total, width)
    own = shape(levels, rows, width)
    ghost = shape(levels * PER_LEVEL, width)
    edges = shape(levels * EDGES, width)
    message = shape(levels, rows + 8, width)
    narrow = shape(-(-levels * (rows + 2) // 8) * 8, width)
    scratch = pltpu.VMEM((levels, total, width), F32)

    w_next_own = over_chips(w)
    first, second, b_e, c_e, w_e, d_e = call(
        pack_kernel,
        [ghost, ghost, field, fields, field, field],
        hbm=True,
        count=6,
        scratch=(
            pltpu.VMEM(obs_pos.shape[1:], jnp.int32),
            pltpu.SMEM(obs_block.shape, jnp.int32),
            pltpu.VMEM(obs_weight.shape[1:], F32),
            pltpu.VMEM((b.size // 128, 128), F32),
            pltpu.SemaphoreType.DMA((6,)),
        ),
    )(*(in_hbm(x) for x in (b, c, w, obs_pos[0], obs_block, obs_weight[0])))
    first = swapped(first, "tile", 0)
    second = swapped(second, "tile", 1)
    (cross_own,) = call(extend_kernel, [own], count=2)(b_e, c_e)
    cross_own = over_chips(cross_own)
    b_e, c_e, w_e, d_e, p0, cross, within = call(
        ghosts_kernel,
        [field, fields, field, field, field, edges, shape(2 * levels, total, width)],
        aliases={2: 0, 3: 1, 4: 2, 5: 3},
        count=6,
    )(first, second, b_e, c_e, w_e, d_e)
    cross, within = exchanged(cross, within)
    q1, p1, w_next, cross, within = call(
        first_apply_kernel,
        [field, field, field, message, message],
        count=9,
        scratch=(scratch,) * 3,
    )(b_e, c_e, w_e, d_e, p0, cross_own, w_next_own, cross, within)
    cross, within = exchanged(cross, within)
    (sums_1,) = call(products_kernel, [shape(3, 8, 128)], count=2)(b_e, q1)
    q2, p2, cross, within = call(
        apply_kernel, [field, field, narrow, narrow], count=8, scratch=(scratch,)
    )(q1, c_e, w_e, d_e, p1, w_next, cross, within)
    cross, within = exchanged(cross, within)
    (sums_2,) = call(products_kernel, [shape(2, 8, 128)], count=2)(q1, q2)
    near, far = ("win_1", "tile"), ("win_0", "win_2")
    moments, q3 = call(
        moments_kernel,
        [shape(lax.axis_size(near), 1, 128), field],
        count=10,
        scratch=(scratch,) + (pltpu.VMEM(narrow.shape, F32),) * 2,
    )(q2, c_e, w_e, d_e, p2, w_next, cross, within, sums_1, sums_2)
    moments = lax.all_to_all(moments, near, 0, 0, tiled=True)
    (moments,) = call(spread_kernel, [shape(lax.axis_size(far), 1, 128)], count=1)(moments)
    moments = lax.all_to_all(moments, far, 0, 0, tiled=True)
    solution_field, residual = call(finish_kernel, [own, own], count=5)(moments, b_e, q1, q2, q3)
    return solution_field[None], residual[None]


def solution(mesh):
    split = Mesh(
        mesh.devices.reshape(8, 8, 2, mesh.shape["tile"]), ("win_0", "win_1", "win_2", "tile")
    )
    in_specs = (
        P(WIN, None, "tile", None),
        P(WIN, None, "tile", None),
        P(None, WIN, None, "tile", None),
        P(WIN, "tile"),
        P(WIN, "tile", None),
        P(WIN, "tile", None),
    )
    out_specs = (P(WIN, None, "tile", None), P(WIN, None, "tile", None))
    return jax.shard_map(solve, mesh=split, in_specs=in_specs, out_specs=out_specs, check_vma=False)
```

```python
import jax
import jax.numpy as jnp
from jax import lax
from jax.experimental import pallas as pl
from jax.experimental.pallas import tpu as pltpu
from jax.sharding import Mesh
from jax.sharding import PartitionSpec as P


WIN = ("win_0", "win_1", "win_2")
THETA = 6.0
G = 8
F32 = jnp.float32


def call(body, out_shape, aliases=None, hbm=False, count=0, scratch=()):
    place = pltpu.HBM if hbm else pltpu.VMEM
    return pl.pallas_call(
        body,
        out_shape=out_shape,
        in_specs=[pl.BlockSpec(memory_space=place) for _ in range(count)],
        out_specs=[pl.BlockSpec(memory_space=pltpu.VMEM) for _ in out_shape],
        scratch_shapes=scratch,
        input_output_aliases=aliases or {},
        compiler_params=pltpu.CompilerParams(vmem_limit_bytes=24 * 2**20),
    )


def in_hbm(x):
    return pltpu.with_memory_space_constraint(x, pltpu.HBM)


def shape(*dims):
    return jax.ShapeDtypeStruct(dims, F32)


def west(x):
    return pltpu.roll(x, 1, axis=1)


def east(x):
    return pltpu.roll(x, x.shape[1] - 1, axis=1)


def north_of(ref, lev, tile):
    if tile == 0:
        return pltpu.roll(ref[lev, 0:8, :], 1, axis=0)
    return ref[lev, 8 * tile - 1 : 8 * tile + 7, :]


def south_of(ref, lev, tile, tiles):
    if tile == tiles - 1:
        return pltpu.roll(ref[lev, 8 * tile : 8 * tile + 8, :], 7, axis=0)
    return ref[lev, 8 * tile + 1 : 8 * tile + 9, :]


def folded(x):
    total = x[:, 0:128]
    for at in range(128, x.shape[1], 128):
        total = total + x[:, at : at + 128]
    return total


PARTS = (("b", 0, 5), ("c", 0, 4), ("c", 1, 5), ("c", 2, 4), ("c", 3, 4), ("w", 0, 5), ("d", 0, 4), ("p", 0, 1))
PER_LEVEL = sum(count for _, _, count in PARTS)
EDGES = 20


def ghost_items(levels):
    at = 0
    for lev in range(levels):
        for name, f, rows in PARTS:
            yield name, f, lev, at, rows
            at += rows


def pack_kernel(
    b_hbm, c_hbm, w_hbm, pos_hbm, block_hbm, weight_hbm,
    north, south, b_e, c_e, w_e, d_e,
    pos, block, weight, blocks, sems,
):
    levels, rows, width = b_hbm.shape
    per_row = width // 128
    own = pl.ds(G, rows)
    pairs = (
        (pos_hbm, pos),
        (weight_hbm, weight),
        (block_hbm, block),
        (b_hbm, b_e.at[:, own, :]),
        (w_hbm, w_e.at[:, own, :]),
        (c_hbm, c_e.at[:, :, own, :]),
    )
    moves = [pltpu.make_async_copy(src, dst, sems.at[i]) for i, (src, dst) in enumerate(pairs)]
    for move in moves:
        move.start()
    blank = jnp.zeros((G, width), F32)
    for lev in range(levels):
        for out in (b_e.at[lev], w_e.at[lev], d_e.at[lev], *(c_e.at[f, lev] for f in range(4))):
            out[0:G, :] = blank
            out[G + rows :, :] = blank
    blocks[...] = jnp.zeros(blocks.shape, F32)
    for move in moves[:3]:
        move.wait()
    hot = block_sums(pos[...].astype(F32), weight[...])
    for i in range(hot.shape[0]):
        at = pl.ds(block[0, i], 1)
        blocks[at, :] = blocks[at, :] + hot[i : i + 1, :]
    for lev in range(levels):
        for j in range(per_row):
            first = lev * rows * per_row + j
            d_e[lev, G : G + rows, j * 128 : j * 128 + 128] = blocks[
                pl.ds(first, rows, stride=per_row), :
            ]
    for move in moves[3:]:
        move.wait()
    for name, f, lev, at, count in ghost_items(levels):
        for out, first in ((north, G), (south, G + rows - count)):
            if name == "p":
                tile = 1 if out is north else rows // 8
                image = model_tile(b_e, c_e, lev, tile, 2 + rows // 8)
                piece = image[4:5, :] if out is north else image[3:4, :]
            else:
                src = {"b": b_e, "c": c_e.at[f], "w": w_e, "d": d_e}[name]
                piece = src[lev, first : first + count, :]
            out[at : at + count, :] = piece


def block_sums(pos, weight):
    n, width = pos.shape
    groups = width // n

    def packed(x):
        turned = x.T
        return jnp.concatenate([turned[g * n : g * n + n, :] for g in range(groups)], axis=1)

    pos, weight = packed(pos), packed(weight)
    cell = lax.broadcasted_iota(jnp.int32, (width, width), 0).astype(F32)
    total = jnp.zeros((width, width), F32)
    for i in range(n):
        here = jnp.broadcast_to(pos[i : i + 1, :], (width, width))
        value = jnp.broadcast_to(weight[i : i + 1, :], (width, width))
        total = total + jnp.where(here == cell, value, 0.0)
    shift = width // 2
    while shift >= n:
        total = total + pltpu.roll(total, shift, axis=1)
        shift //= 2
    return total.T[0:n, :]


def extend_kernel(b_e, c_e, w_e, cross):
    levels, total, _ = b_e.shape
    rows = total - 2 * G
    for lev in range(levels):
        cross[levels + lev, :, :] = w_e[lev, G : G + rows, :]

    @pl.when(core_is_one())
    def _():
        for lev in range(levels):
            for tile in range(1, 1 + rows // 8):
                at = 8 * tile - G
                cross[lev, at : at + 8, :] = model_tile(b_e, c_e, lev, tile, 2 + rows // 8)

    @pl.when(jnp.logical_not(core_is_one()))
    def _():
        for lev in range(levels):
            cross[lev, :, :] = b_e[lev, G : G + rows, :]


def model_tile(q, c, lev, tile, tiles):
    here = q[lev, 8 * tile : 8 * tile + 8, :]
    at = slice(8 * tile, 8 * tile + 8)
    return (
        c[0, lev, at, :] * here
        + c[1, lev, at, :] * (north_of(q, lev, tile) + south_of(q, lev, tile, tiles))
        + c[2, lev, at, :] * east(here)
        + c[3, lev, at, :] * west(here)
    )


def propagate(q, c, p):
    levels, rows, _ = q.shape
    for lev in range(levels):
        for tile in range(rows // 8):
            p[lev, 8 * tile : 8 * tile + 8, :] = model_tile(q, c, lev, tile, rows // 8)


def post(out, values, lev):
    reach = out.shape[1] - (values.shape[1] - 2 * G)
    first = G - reach // 2
    out[lev, :, :] = values[lev, first : first + out.shape[1], :]


def core_is_one():
    return lax.axis_index("win_2") == 1


def ghosts_kernel(from_north, from_south, b_in, c_in, w_in, d_in, b_e, c_e, w_e, d_e, p, cross, within):
    levels, total, width = b_e.shape
    rows = total - 2 * G

    def fill(names):
        for name, f, lev, at, count in ghost_items(levels):
            if name in names:
                out = {"b": b_e, "c": c_e.at[f], "w": w_e, "d": d_e, "p": p}[name]
                reach = 5 if name == "p" else count
                low, high = G - reach, G + rows + reach - count
                out[lev, low : low + count, :] = from_north[at : at + count, :]
                out[lev, high : high + count, :] = from_south[at : at + count, :]

    fill("bcwd")
    propagate(b_e, c_e, p)
    fill("p")

    @pl.when(core_is_one())
    def _():
        for lev in range(levels):
            at = lev * EDGES
            cross[at : at + 5, :] = p[lev, 4:9, :]
            cross[at + 5 : at + 10, :] = p[lev, G + rows - 1 : G + rows + 4, :]
            cross[at + 10 : at + EDGES, :] = jnp.zeros((EDGES - 10, width), F32)
            within[lev] = b_e[lev]
            within[levels + lev] = w_e[lev]

    @pl.when(jnp.logical_not(core_is_one()))
    def _():
        for lev in range(levels):
            for f, field in enumerate((b_e, w_e)):
                low, high = lev * EDGES + 10 * f, lev * EDGES + 10 * f + 5
                cross[low : low + 5, :] = field[lev, 3:8, :]
                cross[high : high + 5, :] = field[lev, G + rows : G + rows + 5, :]
            within[lev] = p[lev]
            within[levels + lev] = p[lev]


def unposted(ref, lev, tile, tiles):
    if tile == 0:
        return pltpu.roll(ref[lev, 0:8, :], 4, axis=0)
    if tile == tiles - 1:
        return pltpu.roll(ref[lev, 8 * tile - 8 : 8 * tile, :], 4, axis=0)
    return ref[lev, 8 * tile - 4 : 8 * tile + 4, :]


def second_half(q, c, w, d, p, v_next, w_next, p_prev, out, edge):
    levels, total, _ = q.shape
    tiles = total // 8
    for lev in range(levels):
        for tile in range(tiles):
            at = slice(8 * tile, 8 * tile + 8)
            here, weight = q[lev, at, :], w[lev, at, :]
            following = w_next(lev, tile) * (v_next(lev, tile) - p[lev, at, :])
            edge[lev, at, :] = c[1, lev, at, :] * following
            out[lev, at, :] = (
                (weight + d[lev, at, :] - THETA) * here
                - weight * p_prev(lev, tile)
                - c[0, lev, at, :] * following
                - west(c[2, lev, at, :] * following)
                - east(c[3, lev, at, :] * following)
            )
    for lev in range(levels):
        for tile in range(tiles):
            at = slice(8 * tile, 8 * tile + 8)
            value = out[lev, at, :] - (north_of(edge, lev, tile) + south_of(edge, lev, tile, tiles))
            if tile in (0, tiles - 1):
                value = jnp.where(w[lev, at, :] > 0.0, value, 0.0)
            out[lev, at, :] = value


def products_kernel(x, y, out):
    levels, total, _ = x.shape
    totals = [jnp.zeros((8, 128), F32) for _ in range(out.shape[0])]
    for lev in range(levels):
        for at in range(G, total - G, 8):
            u, v = x[lev, at : at + 8, :], y[lev, at : at + 8, :]
            for i, (a, b) in enumerate(((u, v), (v, v), (u, u))[: len(totals)]):
                totals[i] = totals[i] + folded(a * b)
    for i, part in enumerate(totals):
        out[i] = part


def send_both(q, p, cross, within):
    def send(forward, backward):
        for lev in range(q.shape[0]):
            post(forward, p, lev)
            post(backward, q, lev)

    @pl.when(core_is_one())
    def _():
        send(cross, within)

    @pl.when(jnp.logical_not(core_is_one()))
    def _():
        send(within, cross)


def first_apply_kernel(
    b_e, c, w, d, p0, cross_own, cross_in, within_in,
    q1, p1, w_next, cross, within, edge, v_next, p_prev,
):
    levels, total, width = b_e.shape
    rows = total - 2 * G
    blank = jnp.zeros((G, width), F32)

    @pl.when(core_is_one())
    def _():
        for lev in range(levels):
            p_prev[lev] = within_in[lev]
            for f, out in enumerate((v_next, w_next)):
                low, high = lev * EDGES + 10 * f, lev * EDGES + 10 * f + 5
                out[lev, 0:G, :] = blank
                out[lev, G : G + rows, :] = cross_own[f * levels + lev]
                out[lev, G + rows :, :] = blank
                out[lev, 3:8, :] = cross_in[low : low + 5, :]
                out[lev, G + rows : G + rows + 5, :] = cross_in[high : high + 5, :]

    @pl.when(jnp.logical_not(core_is_one()))
    def _():
        for lev in range(levels):
            at = lev * EDGES
            v_next[lev] = within_in[lev]
            w_next[lev] = within_in[levels + lev]
            p_prev[lev, 0:G, :] = blank
            p_prev[lev, G : G + rows, :] = cross_own[lev]
            p_prev[lev, G + rows :, :] = blank
            p_prev[lev, 4:9, :] = cross_in[at : at + 5, :]
            p_prev[lev, G + rows - 1 : G + rows + 4, :] = cross_in[at + 5 : at + 10, :]

    def tile_of(ref):
        return lambda lev, tile: ref[lev, 8 * tile : 8 * tile + 8, :]

    second_half(
        b_e, c, w, d, p0, tile_of(v_next), tile_of(w_next), tile_of(p_prev), q1, edge
    )
    propagate(q1, c, p1)
    send_both(q1, p1, cross, within)


def apply_kernel(
    q1, c, w, d, p1, w_next, cross_in, within_in, q2, p2, cross, within, edge
):
    _, total, _ = q1.shape
    tiles = total // 8
    one = core_is_one()

    def v_next(lev, tile):
        return jnp.where(
            one, unposted(cross_in, lev, tile, tiles), unposted(within_in, lev, tile, tiles)
        )

    def p_prev(lev, tile):
        return jnp.where(
            one, unposted(within_in, lev, tile, tiles), unposted(cross_in, lev, tile, tiles)
        )

    second_half(
        q1, c, w, d, p1, v_next,
        lambda lev, tile: w_next[lev, 8 * tile : 8 * tile + 8, :], p_prev, q2, edge,
    )
    propagate(q2, c, p2)
    send_both(q2, p2, cross, within)


def moments_kernel(q2, c, w, d, p2, w_next, cross_in, within_in, sums_1, sums_2, out, q3, edge, v_next, p_prev):
    levels, total, _ = q2.shape
    tiles = total // 8
    one = core_is_one()
    first = jnp.logical_and(
        lax.axis_index("win_0") + lax.axis_index("win_1") == 0, jnp.logical_not(one)
    )

    @pl.when(one)
    def _():
        v_next[...] = cross_in[...]
        p_prev[...] = within_in[...]

    @pl.when(jnp.logical_not(one))
    def _():
        v_next[...] = within_in[...]
        p_prev[...] = cross_in[...]

    last = jnp.zeros((8, 128), F32)
    for lev in range(levels):
        for tile in range(1, tiles - 1):
            at = slice(8 * tile, 8 * tile + 8)
            here, weight = q2[lev, at, :], w[lev, at, :]
            gap = v_next[lev, 8 * tile - 4 : 8 * tile + 4, :] - p2[lev, at, :]
            following = w_next[lev, at, :] * gap
            diagonal = d[lev, at, :] - THETA
            own = diagonal + jnp.where(first, weight, 0.0)
            last = last + folded(following * gap + own * here * here)
            edge[lev, at, :] = c[1, lev, at, :] * following
            q3[lev, at, :] = (
                (weight + diagonal) * here
                - weight * p_prev[lev, 8 * tile - 4 : 8 * tile + 4, :]
                - c[0, lev, at, :] * following
                - west(c[2, lev, at, :] * following)
                - east(c[3, lev, at, :] * following)
            )
        for row, at in ((G - 1, 3), (total - G, total - G - 4)):
            following = w_next[lev, row : row + 1, :] * (
                v_next[lev, at : at + 1, :] - p2[lev, row : row + 1, :]
            )
            edge[lev, row : row + 1, :] = c[1, lev, row : row + 1, :] * following
        for tile in range(1, tiles - 1):
            at = slice(8 * tile, 8 * tile + 8)
            q3[lev, at, :] = q3[lev, at, :] - (
                north_of(edge, lev, tile) + south_of(edge, lev, tile, tiles)
            )
    lane = lax.broadcasted_iota(jnp.int32, (1, 128), 1)
    result = jnp.zeros((1, 128), F32)
    parts = [sums_1[2], sums_1[0], sums_1[1], sums_2[0], sums_2[1], last]
    for i, part in enumerate(parts):
        total_i = jnp.sum(jnp.sum(part, axis=0, keepdims=True), axis=1, keepdims=True)
        result = jnp.where(lane == i, jnp.broadcast_to(total_i, (1, 128)), result)
    for i in range(out.shape[0]):
        out[i] = result


def spread_kernel(x, out):
    total = summed(x)
    for i in range(out.shape[0]):
        out[i] = total


def summed(x):
    parts = [x[i] for i in range(x.shape[0])]
    while len(parts) > 1:
        parts = [a + b for a, b in zip(parts[::2], parts[1::2])]
    return parts[0]


def times_a(v):
    longer = [THETA * x for x in v] + [0.0]
    return [longer[i] + (v[i - 1] if i else 0.0) for i in range(len(longer))]


def inner(u, v, mu):
    return sum(x * y * mu[i + j] for i, x in enumerate(u) for j, y in enumerate(v))


def plus(u, scale, v):
    size = max(len(u), len(v))
    u, v = u + [0.0] * (size - len(u)), v + [0.0] * (size - len(v))
    return [x + scale * y for x, y in zip(u, v)]


def coordinates(mu, iters=3):
    x, r, p = [0.0], [1.0], [1.0]
    rr = mu[0]
    for i in range(iters):
        image = times_a(p)
        alpha = rr / inner(p, image, mu)
        x = plus(x, alpha, p)
        r = plus(r, -alpha, image)
        if i + 1 < iters:
            new = inner(r, r, mu)
            p = plus(r, new / rr, p)
            rr = new
    return x, r


def finish_kernel(parts, q0, q1, q2, q3, solution_field, residual):
    levels, rows, width = solution_field.shape
    total = summed(parts)
    mu = [jnp.broadcast_to(total[:, i : i + 1], (8, 128)) for i in range(6)]
    x, r = coordinates(mu)
    wide = lambda v: jnp.concatenate([v] * (width // 128), axis=1)
    x = [wide(v) for v in x]
    r = [wide(v) for v in r]
    for lev in range(levels):
        for at in range(0, rows, 8):
            s = [q[lev, G + at : G + at + 8, :] for q in (q0, q1, q2, q3)]
            solution_field[lev, at : at + 8, :] = x[0] * s[0] + x[1] * s[1] + x[2] * s[2]
            residual[lev, at : at + 8, :] = r[0] * s[0] + r[1] * s[1] + r[2] * s[2] + r[3] * s[3]


def shifted(x, axis, by):
    count = lax.axis_size(axis)
    return lax.ppermute(x, axis, [(i, i + by) for i in range(count) if 0 <= i + by < count])


def exchanged(cross, within):
    cross = over_chips(cross)
    within = on_chip(within)
    return cross, within


def over_chips(x):
    count = lax.axis_size(WIN)
    pairs = [(i, i + 1) for i in range(1, count - 1, 2)]
    return lax.ppermute(x, WIN, pairs + [(b, a) for a, b in pairs])


def on_chip(x):
    return lax.ppermute(x, "win_2", [(0, 1), (1, 0)])


def solve(right_side, error_weight, coeffs, obs_block, obs_pos, obs_weight):
    b, w, c = right_side[0], error_weight[0], coeffs[:, 0]
    levels, rows, width = b.shape
    total = rows + 2 * G
    field = shape(levels, total, width)
    fields = shape(4, levels, total, width)
    own = shape(levels, rows, width)
    ghost = shape(levels * PER_LEVEL, width)
    edges = shape(levels * EDGES, width)
    message = shape(levels, rows + 8, width)
    scratch = pltpu.VMEM((levels, total, width), F32)

    north, south, b_e, c_e, w_e, d_e = call(
        pack_kernel,
        [ghost, ghost, field, fields, field, field],
        hbm=True,
        count=6,
        scratch=(
            pltpu.VMEM(obs_pos.shape[1:], jnp.int32),
            pltpu.SMEM(obs_block.shape, jnp.int32),
            pltpu.VMEM(obs_weight.shape[1:], F32),
            pltpu.VMEM((b.size // 128, 128), F32),
            pltpu.SemaphoreType.DMA((6,)),
        ),
    )(*(in_hbm(x) for x in (b, c, w, obs_pos[0], obs_block, obs_weight[0])))
    from_south = shifted(north, "tile", -1)
    from_north = shifted(south, "tile", 1)
    (cross_own,) = call(extend_kernel, [shape(2 * levels, rows, width)], count=3)(b_e, c_e, w_e)
    cross_own = over_chips(cross_own)
    b_e, c_e, w_e, d_e, p0, cross, within = call(
        ghosts_kernel,
        [field, fields, field, field, field, edges, shape(2 * levels, total, width)],
        aliases={2: 0, 3: 1, 4: 2, 5: 3},
        count=6,
    )(from_north, from_south, b_e, c_e, w_e, d_e)
    cross, within = exchanged(cross, within)
    q1, p1, w_next, cross, within = call(
        first_apply_kernel,
        [field, field, field, message, message],
        count=8,
        scratch=(scratch,) * 3,
    )(b_e, c_e, w_e, d_e, p0, cross_own, cross, within)
    cross, within = exchanged(cross, within)
    (sums_1,) = call(products_kernel, [shape(3, 8, 128)], count=2)(b_e, q1)
    q2, p2, cross, within = call(
        apply_kernel, [field, field, message, message], count=8, scratch=(scratch,)
    )(q1, c_e, w_e, d_e, p1, w_next, cross, within)
    cross, within = exchanged(cross, within)
    (sums_2,) = call(products_kernel, [shape(2, 8, 128)], count=2)(q1, q2)
    near, far = ("win_0", "win_2"), ("win_1", "tile")
    moments, q3 = call(
        moments_kernel,
        [shape(lax.axis_size(near), 1, 128), field],
        count=10,
        scratch=(scratch,) + (pltpu.VMEM((levels, rows + 8, width), F32),) * 2,
    )(q2, c_e, w_e, d_e, p2, w_next, cross, within, sums_1, sums_2)
    moments = lax.all_to_all(moments, near, 0, 0, tiled=True)
    (moments,) = call(spread_kernel, [shape(lax.axis_size(far), 1, 128)], count=1)(moments)
    moments = lax.all_to_all(moments, far, 0, 0, tiled=True)
    solution_field, residual = call(finish_kernel, [own, own], count=5)(moments, b_e, q1, q2, q3)
    return solution_field[None], residual[None]


def solution(mesh):
    split = Mesh(
        mesh.devices.reshape(8, 8, 2, mesh.shape["tile"]), ("win_0", "win_1", "win_2", "tile")
    )
    in_specs = (
        P(WIN, None, "tile", None),
        P(WIN, None, "tile", None),
        P(None, WIN, None, "tile", None),
        P(WIN, "tile"),
        P(WIN, "tile", None),
        P(WIN, "tile", None),
    )
    out_specs = (P(WIN, None, "tile", None), P(WIN, None, "tile", None))
    return jax.shard_map(solve, mesh=split, in_specs=in_specs, out_specs=out_specs, check_vma=False)
```

```python
import jax
import jax.numpy as jnp
from jax import lax
from jax.experimental import pallas as pl
from jax.experimental.pallas import tpu as pltpu
from jax.sharding import Mesh
from jax.sharding import PartitionSpec as P


WIN = ("win_0", "win_1", "win_2")
THETA = 6.0
G = 8
F32 = jnp.float32


def call(body, out_shape, aliases=None, hbm=False, count=0, scratch=()):
    place = pltpu.HBM if hbm else pltpu.VMEM
    return pl.pallas_call(
        body,
        out_shape=out_shape,
        in_specs=[pl.BlockSpec(memory_space=place) for _ in range(count)],
        out_specs=[pl.BlockSpec(memory_space=pltpu.VMEM) for _ in out_shape],
        scratch_shapes=scratch,
        input_output_aliases=aliases or {},
        compiler_params=pltpu.CompilerParams(vmem_limit_bytes=24 * 2**20),
    )


def in_hbm(x):
    return pltpu.with_memory_space_constraint(x, pltpu.HBM)


def shape(*dims):
    return jax.ShapeDtypeStruct(dims, F32)


def west(x):
    return pltpu.roll(x, 1, axis=1)


def east(x):
    return pltpu.roll(x, x.shape[1] - 1, axis=1)


def north_of(ref, lev, tile):
    if tile == 0:
        return pltpu.roll(ref[lev, 0:8, :], 1, axis=0)
    return ref[lev, 8 * tile - 1 : 8 * tile + 7, :]


def south_of(ref, lev, tile, tiles):
    if tile == tiles - 1:
        return pltpu.roll(ref[lev, 8 * tile : 8 * tile + 8, :], 7, axis=0)
    return ref[lev, 8 * tile + 1 : 8 * tile + 9, :]


def folded(x):
    total = x[:, 0:128]
    for at in range(128, x.shape[1], 128):
        total = total + x[:, at : at + 128]
    return total


PARTS = (("b", 0, 5), ("c", 0, 4), ("c", 1, 5), ("c", 2, 4), ("c", 3, 4), ("w", 0, 5), ("d", 0, 4), ("p", 0, 1))
PER_LEVEL = sum(count for _, _, count in PARTS)
EDGES = 20


def ghost_items(levels):
    at = 0
    for lev in range(levels):
        for name, f, rows in PARTS:
            yield name, f, lev, at, rows
            at += rows


def pack_kernel(
    b_hbm, c_hbm, w_hbm, pos_hbm, block_hbm, weight_hbm,
    north, south, b_e, c_e, w_e, d_e,
    pos, block, weight, blocks, sems,
):
    levels, rows, width = b_hbm.shape
    per_row = width // 128
    own = pl.ds(G, rows)
    pairs = (
        (pos_hbm, pos),
        (weight_hbm, weight),
        (block_hbm, block),
        (b_hbm, b_e.at[:, own, :]),
        (w_hbm, w_e.at[:, own, :]),
        (c_hbm, c_e.at[:, :, own, :]),
    )
    moves = [pltpu.make_async_copy(src, dst, sems.at[i]) for i, (src, dst) in enumerate(pairs)]
    for move in moves:
        move.start()
    blank = jnp.zeros((G, width), F32)
    for lev in range(levels):
        for out in (b_e.at[lev], w_e.at[lev], d_e.at[lev], *(c_e.at[f, lev] for f in range(4))):
            out[0:G, :] = blank
            out[G + rows :, :] = blank
    blocks[...] = jnp.zeros(blocks.shape, F32)
    for move in moves[:3]:
        move.wait()
    hot = block_sums(pos[...].astype(F32), weight[...])
    for i in range(hot.shape[0]):
        at = pl.ds(block[0, i], 1)
        blocks[at, :] = blocks[at, :] + hot[i : i + 1, :]
    for lev in range(levels):
        for j in range(per_row):
            first = lev * rows * per_row + j
            d_e[lev, G : G + rows, j * 128 : j * 128 + 128] = blocks[
                pl.ds(first, rows, stride=per_row), :
            ]
    for move in moves[3:]:
        move.wait()
    for name, f, lev, at, count in ghost_items(levels):
        for out, first in ((north, G), (south, G + rows - count)):
            if name == "p":
                tile = 1 if out is north else rows // 8
                image = model_tile(b_e, c_e, lev, tile, 2 + rows // 8)
                piece = image[4:5, :] if out is north else image[3:4, :]
            else:
                src = {"b": b_e, "c": c_e.at[f], "w": w_e, "d": d_e}[name]
                piece = src[lev, first : first + count, :]
            out[at : at + count, :] = piece


def block_sums(pos, weight):
    n, width = pos.shape
    groups = width // n

    def packed(x):
        turned = x.T
        return jnp.concatenate([turned[g * n : g * n + n, :] for g in range(groups)], axis=1)

    pos, weight = packed(pos), packed(weight)
    cell = lax.broadcasted_iota(jnp.int32, (width, width), 0).astype(F32)
    total = jnp.zeros((width, width), F32)
    for i in range(n):
        here = jnp.broadcast_to(pos[i : i + 1, :], (width, width))
        value = jnp.broadcast_to(weight[i : i + 1, :], (width, width))
        total = total + jnp.where(here == cell, value, 0.0)
    shift = width // 2
    while shift >= n:
        total = total + pltpu.roll(total, shift, axis=1)
        shift //= 2
    return total.T[0:n, :]


def extend_kernel(b_e, c_e, w_e, cross):
    levels, total, _ = b_e.shape
    rows = total - 2 * G
    for lev in range(levels):
        cross[levels + lev, :, :] = w_e[lev, G : G + rows, :]

    @pl.when(core_is_one())
    def _():
        for lev in range(levels):
            for tile in range(1, 1 + rows // 8):
                at = 8 * tile - G
                cross[lev, at : at + 8, :] = model_tile(b_e, c_e, lev, tile, 2 + rows // 8)

    @pl.when(jnp.logical_not(core_is_one()))
    def _():
        for lev in range(levels):
            cross[lev, :, :] = b_e[lev, G : G + rows, :]


def model_tile(q, c, lev, tile, tiles):
    here = q[lev, 8 * tile : 8 * tile + 8, :]
    at = slice(8 * tile, 8 * tile + 8)
    return (
        c[0, lev, at, :] * here
        + c[1, lev, at, :] * (north_of(q, lev, tile) + south_of(q, lev, tile, tiles))
        + c[2, lev, at, :] * east(here)
        + c[3, lev, at, :] * west(here)
    )


def propagate(q, c, p):
    levels, rows, _ = q.shape
    for lev in range(levels):
        for tile in range(rows // 8):
            p[lev, 8 * tile : 8 * tile + 8, :] = model_tile(q, c, lev, tile, rows // 8)


def post(out, values, lev):
    reach = out.shape[1] - (values.shape[1] - 2 * G)
    first = G - reach // 2
    out[lev, :, :] = values[lev, first : first + out.shape[1], :]


def core_is_one():
    return lax.axis_index("win_2") == 1


def by_core(on_one, on_zero):
    pl.when(core_is_one())(on_one)
    pl.when(jnp.logical_not(core_is_one()))(on_zero)


def tile_of(ref):
    return lambda lev, tile: ref[lev, 8 * tile : 8 * tile + 8, :]


def ghosts_kernel(from_north, from_south, b_in, c_in, w_in, d_in, b_e, c_e, w_e, d_e, p, cross, within):
    levels, total, width = b_e.shape
    rows = total - 2 * G

    def fill(names):
        for name, f, lev, at, count in ghost_items(levels):
            if name in names:
                out = {"b": b_e, "c": c_e.at[f], "w": w_e, "d": d_e, "p": p}[name]
                reach = 5 if name == "p" else count
                low, high = G - reach, G + rows + reach - count
                out[lev, low : low + count, :] = from_north[at : at + count, :]
                out[lev, high : high + count, :] = from_south[at : at + count, :]

    fill("bcwd")
    propagate(b_e, c_e, p)
    fill("p")

    @pl.when(core_is_one())
    def _():
        for lev in range(levels):
            at = lev * EDGES
            cross[at : at + 5, :] = p[lev, 4:9, :]
            cross[at + 5 : at + 10, :] = p[lev, G + rows - 1 : G + rows + 4, :]
            cross[at + 10 : at + EDGES, :] = jnp.zeros((EDGES - 10, width), F32)
            within[lev] = b_e[lev]
            within[levels + lev] = w_e[lev]

    @pl.when(jnp.logical_not(core_is_one()))
    def _():
        for lev in range(levels):
            for f, field in enumerate((b_e, w_e)):
                low, high = lev * EDGES + 10 * f, lev * EDGES + 10 * f + 5
                cross[low : low + 5, :] = field[lev, 3:8, :]
                cross[high : high + 5, :] = field[lev, G + rows : G + rows + 5, :]
            within[lev] = p[lev]
            within[levels + lev] = p[lev]


def second_half(q, c, w, d, p, v_next, w_next, p_prev, out, edge):
    levels, total, _ = q.shape
    tiles = total // 8
    for lev in range(levels):
        for tile in range(tiles):
            at = slice(8 * tile, 8 * tile + 8)
            here, weight = q[lev, at, :], w[lev, at, :]
            following = w_next(lev, tile) * (v_next(lev, tile) - p[lev, at, :])
            edge[lev, at, :] = c[1, lev, at, :] * following
            out[lev, at, :] = (
                (weight + d[lev, at, :] - THETA) * here
                - weight * p_prev(lev, tile)
                - c[0, lev, at, :] * following
                - west(c[2, lev, at, :] * following)
                - east(c[3, lev, at, :] * following)
            )
    for lev in range(levels):
        for tile in range(tiles):
            at = slice(8 * tile, 8 * tile + 8)
            value = out[lev, at, :] - (north_of(edge, lev, tile) + south_of(edge, lev, tile, tiles))
            if tile in (0, tiles - 1):
                value = jnp.where(w[lev, at, :] > 0.0, value, 0.0)
            out[lev, at, :] = value


def products_kernel(x, y, out):
    levels, total, _ = x.shape
    totals = [jnp.zeros((8, 128), F32) for _ in range(out.shape[0])]
    for lev in range(levels):
        for at in range(G, total - G, 8):
            u, v = x[lev, at : at + 8, :], y[lev, at : at + 8, :]
            for i, (a, b) in enumerate(((u, v), (v, v), (u, u))[: len(totals)]):
                totals[i] = totals[i] + folded(a * b)
    for i, part in enumerate(totals):
        out[i] = part


def send_both(q, p, cross, within):
    def send(forward, backward):
        for lev in range(q.shape[0]):
            post(forward, p, lev)
            post(backward, q, lev)

    @pl.when(core_is_one())
    def _():
        send(cross, within)

    @pl.when(jnp.logical_not(core_is_one()))
    def _():
        send(within, cross)


def first_apply_kernel(
    b_e, c, w, d, p0, cross_own, cross_in, within_in,
    q1, p1, w_next, cross, within, edge, v_next, p_prev,
):
    levels, total, width = b_e.shape
    rows = total - 2 * G
    blank = jnp.zeros((G, width), F32)

    @pl.when(core_is_one())
    def _():
        for lev in range(levels):
            p_prev[lev] = within_in[lev]
            for f, out in enumerate((v_next, w_next)):
                low, high = lev * EDGES + 10 * f, lev * EDGES + 10 * f + 5
                out[lev, 0:G, :] = blank
                out[lev, G : G + rows, :] = cross_own[f * levels + lev]
                out[lev, G + rows :, :] = blank
                out[lev, 3:8, :] = cross_in[low : low + 5, :]
                out[lev, G + rows : G + rows + 5, :] = cross_in[high : high + 5, :]

    @pl.when(jnp.logical_not(core_is_one()))
    def _():
        for lev in range(levels):
            at = lev * EDGES
            v_next[lev] = within_in[lev]
            w_next[lev] = within_in[levels + lev]
            p_prev[lev, 0:G, :] = blank
            p_prev[lev, G : G + rows, :] = cross_own[lev]
            p_prev[lev, G + rows :, :] = blank
            p_prev[lev, 4:9, :] = cross_in[at : at + 5, :]
            p_prev[lev, G + rows - 1 : G + rows + 4, :] = cross_in[at + 5 : at + 10, :]

    second_half(
        b_e, c, w, d, p0, tile_of(v_next), tile_of(w_next), tile_of(p_prev), q1, edge
    )
    propagate(q1, c, p1)
    send_both(q1, p1, cross, within)


def apply_kernel(
    q1, c, w, d, p1, w_next, cross_in, within_in,
    q2, p2, early, late, within, edge, v_next, p_prev,
):
    levels, total, width = q1.shape
    rows = total - 2 * G

    def assemble(state, image):
        for lev in range(levels):
            for out, src in ((v_next, state), (p_prev, image)):
                out[lev, 0:8, :] = jnp.zeros((8, width), F32)
                out[lev, total - 8 :, :] = jnp.zeros((8, width), F32)
                out[lev, 4 : total - 4, :] = src[lev]

    by_core(lambda: assemble(cross_in, within_in), lambda: assemble(within_in, cross_in))
    second_half(
        q1, c, w, d, p1, tile_of(v_next), tile_of(w_next), tile_of(p_prev), q2, edge
    )
    propagate(q2, c, p2)

    def send_up():
        early[...] = p2[1, G : G + rows, :]
        late[0:rows, :] = p2[0, G : G + rows, :]
        late[rows:, :] = jnp.zeros((late.shape[0] - rows, width), F32)
        for lev in range(levels):
            post(within, q2, lev)

    def send_down():
        early[...] = q2[0, G : G + rows, :]
        late[0 : rows + 2, :] = q2[1, G - 1 : G + rows + 1, :]
        late[rows + 2 : rows + 3, :] = q2[0, G - 1 : G, :]
        late[rows + 3 : rows + 4, :] = q2[0, G + rows : G + rows + 1, :]
        late[rows + 4 :, :] = jnp.zeros((late.shape[0] - rows - 4, width), F32)
        for lev in range(levels):
            post(within, p2, lev)

    by_core(send_up, send_down)


def moments_kernel(q2, w, d, p2, w_next, early_in, within_in, sums_1, sums_2, out, last):
    levels, total, _ = q2.shape
    rows = total - 2 * G
    opening = lax.axis_index("win_0") + lax.axis_index("win_1") == 0

    def sum_of(term):
        amount = jnp.zeros((8, 128), F32)
        for at in range(0, rows, 8):
            amount = amount + folded(term(at, slice(G + at, G + at + 8)))
        return amount

    def squared(weight, gap):
        return weight * gap * gap

    base = jnp.zeros((8, 128), F32)
    for lev in range(levels):
        base = base + sum_of(lambda at, own: squared(d[lev, own, :] - THETA, q2[lev, own, :]))

    def on_one():
        last[...] = base + sum_of(
            lambda at, own: squared(w_next[0, own, :], early_in[at : at + 8, :] - p2[0, own, :])
        )

    def on_zero():
        amount = base + sum_of(
            lambda at, own: squared(w[1, own, :], q2[1, own, :] - early_in[at : at + 8, :])
        )
        for lev in range(levels):
            amount = amount + sum_of(
                lambda at, own: squared(
                    w_next[lev, own, :], within_in[lev, at + 4 : at + 12, :] - p2[lev, own, :]
                )
            )
        first = sum_of(lambda at, own: squared(w[0, own, :], q2[0, own, :]))
        last[...] = amount + jnp.where(opening, first, 0.0)

    by_core(on_one, on_zero)
    lane = lax.broadcasted_iota(jnp.int32, (1, 128), 1)
    result = jnp.zeros((1, 128), F32)
    parts = [sums_1[2], sums_1[0], sums_1[1], sums_2[0], sums_2[1], last[...]]
    for i, part in enumerate(parts):
        total_i = jnp.sum(jnp.sum(part, axis=0, keepdims=True), axis=1, keepdims=True)
        result = jnp.where(lane == i, jnp.broadcast_to(total_i, (1, 128)), result)
    for i in range(out.shape[0]):
        out[i] = result


def spread_kernel(
    x, q2, c, w, d, p2, w_next, early_in, late_in, within_in,
    out, q3, edge, v_next, p_prev,
):
    levels, total, _ = q2.shape
    rows = total - 2 * G
    tiles = total // 8
    for i in range(out.shape[0]):
        out[i] = x[0]

    def on_one():
        v_next[0, G : G + rows, :] = early_in[...]
        v_next[0, G - 1 : G, :] = late_in[rows + 2 : rows + 3, :]
        v_next[0, G + rows : G + rows + 1, :] = late_in[rows + 3 : rows + 4, :]
        v_next[1, G - 1 : G + rows + 1, :] = late_in[0 : rows + 2, :]
        for lev in range(levels):
            p_prev[lev, :, :] = within_in[lev, 4 : 4 + rows, :]

    def on_zero():
        p_prev[0, :, :] = late_in[0:rows, :]
        p_prev[1, :, :] = early_in[...]
        for lev in range(levels):
            v_next[lev, 4 : total - 4, :] = within_in[lev]

    by_core(on_one, on_zero)
    for lev in range(levels):
        for at in (slice(G - 1, G), slice(G + rows, G + rows + 1)):
            following = w_next[lev, at, :] * (v_next[lev, at, :] - p2[lev, at, :])
            edge[lev, at, :] = c[1, lev, at, :] * following
        for tile in range(1, tiles - 1):
            at, own = slice(8 * tile, 8 * tile + 8), slice(8 * tile - G, 8 * tile - G + 8)
            weight = w[lev, at, :]
            following = w_next[lev, at, :] * (v_next[lev, at, :] - p2[lev, at, :])
            edge[lev, at, :] = c[1, lev, at, :] * following
            q3[lev, own, :] = (
                (weight + d[lev, at, :] - THETA) * q2[lev, at, :]
                - weight * p_prev[lev, own, :]
                - c[0, lev, at, :] * following
                - west(c[2, lev, at, :] * following)
                - east(c[3, lev, at, :] * following)
            )
        for tile in range(1, tiles - 1):
            own = slice(8 * tile - G, 8 * tile - G + 8)
            q3[lev, own, :] = q3[lev, own, :] - (
                north_of(edge, lev, tile) + south_of(edge, lev, tile, tiles)
            )


def total_kernel(x, out):
    out[0] = summed(x)


def summed(x):
    parts = [x[i] for i in range(x.shape[0])]
    while len(parts) > 1:
        parts = [a + b for a, b in zip(parts[::2], parts[1::2])]
    return parts[0]


def times_a(v):
    longer = [THETA * x for x in v] + [0.0]
    return [longer[i] + (v[i - 1] if i else 0.0) for i in range(len(longer))]


def inner(u, v, mu):
    return sum(x * y * mu[i + j] for i, x in enumerate(u) for j, y in enumerate(v))


def plus(u, scale, v):
    size = max(len(u), len(v))
    u, v = u + [0.0] * (size - len(u)), v + [0.0] * (size - len(v))
    return [x + scale * y for x, y in zip(u, v)]


def coordinates(mu, iters=3):
    x, r, p = [0.0], [1.0], [1.0]
    rr = mu[0]
    for i in range(iters):
        image = times_a(p)
        alpha = rr / inner(p, image, mu)
        x = plus(x, alpha, p)
        r = plus(r, -alpha, image)
        if i + 1 < iters:
            new = inner(r, r, mu)
            p = plus(r, new / rr, p)
            rr = new
    return x, r


def finish_kernel(parts, q0, q1, q2, q3, solution_field, residual):
    levels, rows, width = solution_field.shape
    total = summed(parts)
    mu = [jnp.broadcast_to(total[:, i : i + 1], (8, 128)) for i in range(6)]
    x, r = coordinates(mu)
    wide = lambda v: jnp.concatenate([v] * (width // 128), axis=1)
    x = [wide(v) for v in x]
    r = [wide(v) for v in r]
    for lev in range(levels):
        for at in range(0, rows, 8):
            s = [q[lev, G + at : G + at + 8, :] for q in (q0, q1, q2)]
            last = q3[lev, at : at + 8, :]
            solution_field[lev, at : at + 8, :] = x[0] * s[0] + x[1] * s[1] + x[2] * s[2]
            residual[lev, at : at + 8, :] = r[0] * s[0] + r[1] * s[1] + r[2] * s[2] + r[3] * last


def shifted(x, axis, by):
    count = lax.axis_size(axis)
    return lax.ppermute(x, axis, [(i, i + by) for i in range(count) if 0 <= i + by < count])


def exchanged(cross, within):
    cross = over_chips(cross)
    within = on_chip(within)
    return cross, within


def over_chips(x):
    count = lax.axis_size(WIN)
    pairs = [(i, i + 1) for i in range(1, count - 1, 2)]
    return lax.ppermute(x, WIN, pairs + [(b, a) for a, b in pairs])


def on_chip(x):
    return lax.ppermute(x, "win_2", [(0, 1), (1, 0)])


def solve(right_side, error_weight, coeffs, obs_block, obs_pos, obs_weight):
    b, w, c = right_side[0], error_weight[0], coeffs[:, 0]
    levels, rows, width = b.shape
    total = rows + 2 * G
    field = shape(levels, total, width)
    fields = shape(4, levels, total, width)
    own = shape(levels, rows, width)
    ghost = shape(levels * PER_LEVEL, width)
    edges = shape(levels * EDGES, width)
    message = shape(levels, rows + 8, width)
    scratch = pltpu.VMEM((levels, total, width), F32)

    north, south, b_e, c_e, w_e, d_e = call(
        pack_kernel,
        [ghost, ghost, field, fields, field, field],
        hbm=True,
        count=6,
        scratch=(
            pltpu.VMEM(obs_pos.shape[1:], jnp.int32),
            pltpu.SMEM(obs_block.shape, jnp.int32),
            pltpu.VMEM(obs_weight.shape[1:], F32),
            pltpu.VMEM((b.size // 128, 128), F32),
            pltpu.SemaphoreType.DMA((6,)),
        ),
    )(*(in_hbm(x) for x in (b, c, w, obs_pos[0], obs_block, obs_weight[0])))
    from_south = shifted(north, "tile", -1)
    from_north = shifted(south, "tile", 1)
    (cross_own,) = call(extend_kernel, [shape(2 * levels, rows, width)], count=3)(b_e, c_e, w_e)
    cross_own = over_chips(cross_own)
    b_e, c_e, w_e, d_e, p0, cross, within = call(
        ghosts_kernel,
        [field, fields, field, field, field, edges, shape(2 * levels, total, width)],
        aliases={2: 0, 3: 1, 4: 2, 5: 3},
        count=6,
    )(from_north, from_south, b_e, c_e, w_e, d_e)
    cross, within = exchanged(cross, within)
    q1, p1, w_next, cross, within = call(
        first_apply_kernel,
        [field, field, field, message, message],
        count=8,
        scratch=(scratch,) * 3,
    )(b_e, c_e, w_e, d_e, p0, cross_own, cross, within)
    cross, within = exchanged(cross, within)
    (sums_1,) = call(products_kernel, [shape(3, 8, 128)], count=2)(b_e, q1)
    q2, p2, early, late, within = call(
        apply_kernel,
        [field, field, shape(rows, width), shape(rows + 8, width), message],
        count=8,
        scratch=(scratch,) * 3,
    )(q1, c_e, w_e, d_e, p1, w_next, cross, within)
    early = over_chips(early)
    within = on_chip(within)
    late = over_chips(late)
    (sums_2,) = call(products_kernel, [shape(2, 8, 128)], count=2)(q1, q2)
    near, far = ("win_0", "win_2"), ("win_1", "tile")
    (moments,) = call(
        moments_kernel,
        [shape(lax.axis_size(near), 1, 128)],
        count=9,
        scratch=(pltpu.VMEM((8, 128), F32),),
    )(q2, w_e, d_e, p2, w_next, early, within, sums_1, sums_2)
    moments = lax.all_to_all(moments, near, 0, 0, tiled=True)
    (moments,) = call(total_kernel, [shape(1, 1, 128)], count=1)(moments)
    moments, q3 = call(
        spread_kernel,
        [shape(lax.axis_size(far), 1, 128), own],
        count=10,
        scratch=(scratch, scratch, pltpu.VMEM((levels, rows, width), F32)),
    )(moments, q2, c_e, w_e, d_e, p2, w_next, early, late, within)
    moments = lax.all_to_all(moments, far, 0, 0, tiled=True)
    solution_field, residual = call(finish_kernel, [own, own], count=5)(moments, b_e, q1, q2, q3)
    return solution_field[None], residual[None]


def solution(mesh):
    split = Mesh(
        mesh.devices.reshape(8, 8, 2, mesh.shape["tile"]), ("win_0", "win_1", "win_2", "tile")
    )
    in_specs = (
        P(WIN, None, "tile", None),
        P(WIN, None, "tile", None),
        P(None, WIN, None, "tile", None),
        P(WIN, "tile"),
        P(WIN, "tile", None),
        P(WIN, "tile", None),
    )
    out_specs = (P(WIN, None, "tile", None), P(WIN, None, "tile", None))
    return jax.shard_map(solve, mesh=split, in_specs=in_specs, out_specs=out_specs, check_vma=False)
```
